32 devices in a mesh: band: 2 (over x), tm: 16 (over z, y, core).
Axes of the slice: x: 2, y: 2, z: 4, core: 2. Of those that a mesh axis runs over, the one named last changes fastest.
Arguments:
- voltages: bfloat16 [16, 2, 512, 4096], P('band', None, None, 'tm'), parts along dimension 0, may hold values from -12 to 12
- antenna_flags: int32 [32, 16], P('tm', 'band'), parts along dimension 1, may hold values from -2147483648 to 2147483647, as said below
- owned_tile: int32 [16], replicated, may hold values from 0 to 15, each once
Outputs:
- visibility: float32 [512, 16, 2, 512], P('tm', 'band'), parts along dimension 1
The draws below stay inside these ranges and needn't reach their ends.
There are 2 independent parts, one for each index of `band`. The reference program is written for one: setup_inputs(seed, part) draws one part's arguments, and reference() takes and returns one part's arrays. A program takes and returns all parts, laid end to end along the dimension named above; an argument that names none is the same for every part. Nothing has to cross between parts.
Inputs may be any that keep to these rules, and one draw needn't show every extreme that they name: `antenna_flags`: bit b of word w of sub-integration s is 1 where the samples of both polarisations of antenna 32 * w + b are good in that sub-integration of 128 samples, 0 where flagged; all 32 bits of a word are used; some antennas may be flagged in every sub-integration. A permutation: the index k of tm holds the baseline rows of tile owned_tile[k].
All inputs are finite; a program needn't handle non-finite values.
Results may differ from the reference program's by a relative error of at most 0.0003.
Values sent between devices are 32-bit elements; how exact they have to be, the bound alone decides.
A program may use at most 128 MiB of HBM per device.

```python
import math
import jax
import jax.numpy as jnp
from jax import lax

ANTENNAS = 256
INPUTS = 512
FLAG_WORDS = 8
CHANS = 8
SAMPLES_DEV = 256
SUB_LEN = 128
SUBS = 32
TIME = 4096
TILES = 16
N_TM = 16


def gains(key, lowest, highest):
    key_amplitude, key_phase = jax.random.split(key)
    amplitude = jnp.exp(jax.random.uniform(key_amplitude, (INPUTS,), jnp.float32, math.log(lowest), math.log(highest)))
    phase = jax.random.uniform(key_phase, (INPUTS,), jnp.float32, -math.pi, math.pi)
    return (amplitude * jnp.cos(phase), amplitude * jnp.sin(phase))


def source_term(key, lowest, highest):
    key_sky, key_gain = jax.random.split(key)
    sky = jax.random.normal(key_sky, (CHANS, 2, 1, TIME), jnp.float32)
    gain_real, gain_imag = gains(key_gain, lowest, highest)
    gain_real = gain_real[None, :, None]
    gain_imag = gain_imag[None, :, None]
    real_term = gain_real * sky[:, 0] - gain_imag * sky[:, 1]
    imag_term = gain_real * sky[:, 1] + gain_imag * sky[:, 0]
    return jnp.stack([real_term, imag_term], axis=1)


def draw_voltages(key, part):
    key_first = jax.random.fold_in(jax.random.fold_in(key, 11), 0)
    key_noise = jax.random.fold_in(jax.random.fold_in(key, 11), 2)
    noise = jax.random.normal(key_noise, (CHANS, 2, INPUTS, TIME), jnp.float32)
    signal = source_term(key_first, 0.5, 2.0)
    return jnp.clip(signal + noise, -12.0, 12.0).astype(jnp.bfloat16)


def draw_antenna_flags(key, part):
    key_rolled, key_dead = jax.random.split(jax.random.fold_in(key, 23))
    sub_position = jnp.arange(SUBS, dtype=jnp.int32)[:, None]
    threshold = 30 + 60 * sub_position // max(SUBS - 1, 1)
    rolled = jax.random.randint(key_rolled, (SUBS, ANTENNAS), 0, 100)
    ranking = jax.random.permutation(key_dead, ANTENNAS)
    alive = ranking >= max(1, ANTENNAS // 64)
    bits = jnp.where(alive[None, :] & (rolled < threshold), 1, 0).astype(jnp.int32)
    bits = bits.reshape(SUBS, FLAG_WORDS, 32)
    shifts = jnp.arange(32, dtype=jnp.int32)
    return jnp.sum(jnp.left_shift(bits, shifts[None, None, :]), axis=-1, dtype=jnp.int32)


def setup_inputs(seed: int = 0, part: int = 0) -> dict:
    key_list = jax.random.split(jax.random.key(seed), 4)
    own_keys = jax.random.split(jax.random.fold_in(key_list[3], part), 4)
    voltages = draw_voltages(jax.random.fold_in(jax.random.fold_in(key_list[3], part), 71), part)
    antenna_flags = draw_antenna_flags(jax.random.fold_in(jax.random.fold_in(key_list[3], part), 71), part)
    owned_tile = jax.random.permutation(key_list[2], TILES).astype(jnp.int32)
    return {"voltages": voltages, "antenna_flags": antenna_flags, "owned_tile": owned_tile}


def unpack_flags(words):
    shifts = jnp.arange(32, dtype=jnp.int32)
    bits = jnp.bitwise_and(jnp.right_shift(words[:, :, None], shifts[None, None, :]), 1)
    return bits.reshape(words.shape[0], words.shape[1] * 32).astype(jnp.int32)


def reference(voltages, antenna_flags, owned_tile):
    channels = voltages.shape[0]
    inputs = voltages.shape[2]
    block_rows = inputs // N_TM
    good = unpack_flags(antenna_flags)
    input_flags = jnp.repeat(good, 2, axis=1)
    sample_flags = jnp.repeat(input_flags.T, SUB_LEN, axis=1).astype(jnp.bfloat16)
    masked = voltages * sample_flags[None, None]

    def add_block(running, block_index):
        segment = lax.dynamic_slice_in_dim(masked, block_index * SAMPLES_DEV, SAMPLES_DEV, 3).astype(jnp.float32)
        real_part = segment[:, 0]
        imag_part = segment[:, 1]
        right_side = jnp.concatenate([real_part, imag_part], axis=-1)
        left_side = jnp.stack([right_side, jnp.concatenate([imag_part, -real_part], axis=-1)], axis=1)
        return running + jnp.einsum("ckiu,cju->ckij", left_side, right_side), None

    initial = jnp.zeros((channels, 2, inputs, inputs), jnp.float32)
    gram = lax.scan(add_block, initial, jnp.arange(N_TM, dtype=jnp.int32))[0]
    counts = SUB_LEN * jnp.dot(good.T, good)
    row_index = (owned_tile[:, None] * block_rows + jnp.arange(block_rows, dtype=jnp.int32)[None, :]).reshape(-1)
    pair_counts = jnp.repeat(jnp.repeat(counts, 2, axis=0), 2, axis=1)[row_index]
    ordered = jnp.transpose(gram[:, :, row_index, :], (2, 0, 1, 3))
    return ordered / jnp.maximum(pair_counts, 1).astype(jnp.float32)[:, None, None, :]
```

```python
import functools

import jax
import jax.numpy as jnp
from jax import lax
from jax.experimental import pallas as pl
from jax.experimental.pallas import tpu as pltpu
from jax.sharding import PartitionSpec as P

MESH = pl.DeviceIdType.MESH
CORES = 2
BLOCK = 1.42
HOP = 2.0
FIRST = 6.5
STATIC = 4


def grid_of(mesh):
    count = mesh.shape["tm"]
    ny = 2 if mesh.shape["band"] < 4 and count % (4 * CORES) == 0 else 1
    return count // (ny * CORES), ny


def far_first(nz):
    order = []
    low, high = 0, nz - 1
    while low <= high:
        order.append(low)
        if high > low:
            order.append(high)
        low, high = low + 1, high - 1
    return order


def when(condition, act):
    if isinstance(condition, bool):
        if condition:
            act()
    else:
        pl.when(condition)(act)


def plan(nz, ny, chans, wide):
    merged, order = {}, far_first(nz)
    clock = FIRST
    for ch in range(chans):
        for d in order:
            if ch in wide or ny == 1:
                merged[ch, d] = FIRST - HOP + 0.9 * ch
            else:
                clock += BLOCK
                merged[ch, d] = clock + HOP
    items = [(ch, s, d) for ch in range(chans) for d in order for s in range(ny if ch in wide else 1)]
    events = [[] for _ in range(nz)]
    ends = [dict() for _ in range(nz)]
    for z in range(nz):
        for ch in range(chans):
            ends[z][ch] = [merged[ch, z]] * 2
            if ch not in wide and ny > 1:
                for d in order:
                    events[z].append((merged[ch, d], "merge", (ch, d)))
    for way in range(2):
        arrived = {}
        line = range(nz) if way == 0 else range(nz - 1, -1, -1)
        for place, z in enumerate(line):
            queue = []
            for item in items:
                ch, s, d = item
                if (d < z and way == 0) or (d > z and way == 1):
                    continue
                ready = max(merged[ch, d], arrived.get(item, 0.0))
                if place > 0:
                    events[z].append((ready + 0.001, "chain", (ch, s, d, way)))
                if d == z:
                    ends[z][ch][s] = max(ends[z][ch][s], ready + 0.002)
                else:
                    queue.append((ready, item))
            free = 0.0
            arrived = {}
            for ready, item in sorted(queue):
                free = max(free, ready) + BLOCK
                arrived[item] = free + HOP
    for z in range(nz):
        for ch in range(chans):
            own, other = ends[z][ch]
            if ch in wide:
                events[z].append((other + 0.003, "cross", (ch,)))
                own = max(own, max(other, clock) + BLOCK + HOP)
            events[z].append((own + 0.004, "finish", (ch,)))
        events[z].sort(key=lambda event: event[0])
    return events


def kernel(nz, ny, wide, owned, flags, packed, volts, kept, mirrored, scale, loaded, words_all, mask, natural, left,
           gram, from_core, from_y, from_z, turned, folded, pairs, gathered,
           ls, cs, cr, ys, yr, zs, zr, fs, fr, gs, gr, ks, os):
    count = nz * ny * CORES
    chans, _, tiles, rows, samples = volts.shape
    inputs = tiles * rows
    pack, width = turned.shape[2:]
    me = lax.axis_index("tm")
    core = lax.rem(me, CORES)
    y = lax.rem(me // CORES, ny)
    z = me // (CORES * ny)

    def index_at(zz, yy, cc):
        return (zz * ny + yy) * CORES + cc

    barrier = pltpu.get_barrier_semaphore()

    def greet(target):
        pl.semaphore_signal(barrier, inc=1, device_id={"tm": target}, device_id_type=MESH)

    greet(index_at(z, y, 1 - core))
    if ny > 1:
        greet(index_at(z, 1 - y, core))
    pl.when(z > 0)(lambda: greet(index_at(z - 1, y, core)))
    pl.when(z < nz - 1)(lambda: greet(index_at(z + 1, y, core)))

    def load(ch):
        return pltpu.make_async_copy(volts.at[ch], loaded.at[ch], ls.at[ch])

    for ch in range(chans):
        load(ch).start()

    subs, words = flags.shape
    length = samples // subs
    span = inputs // words
    shift = lax.broadcasted_iota(jnp.int32, (span, length), 0) // 2
    for word in range(words):
        for sub in range(subs):
            bits = jnp.right_shift(jnp.full((span, length), flags[sub, word], jnp.int32), shift)
            good = jnp.bitwise_and(bits, 1).astype(jnp.float32).astype(mask.dtype)
            good = good.reshape(span // rows, rows, length)
            mask[word * (span // rows) : (word + 1) * (span // rows), :, sub * length : (sub + 1) * length] = good

    def remote(src, dst, send, recv, target):
        return pltpu.make_async_remote_copy(
            src_ref=src, dst_ref=dst, send_sem=send, recv_sem=recv,
            device_id={"tm": target}, device_id_type=MESH,
        )

    def core_copy(ch):
        return remote(gram.at[ch, 1 - core], from_core.at[ch], cs.at[ch], cr.at[ch], index_at(z, y, 1 - core))

    def y_copy(ch, d):
        return remote(
            gram.at[ch, core, 1 - y, d], from_y.at[ch, d], ys.at[ch, d], yr.at[ch, d], index_at(z, 1 - y, core)
        )

    def cross_copy(ch):
        return remote(
            gram.at[ch, core, 1 - y, z], from_y.at[ch, 0], ys.at[ch, 0], yr.at[ch, 0], index_at(z, 1 - y, core)
        )

    def block(ch, s, d):
        return gram.at[ch, core, lax.rem(y + s, ny) if ny > 1 else 0, d]

    def z_copy(ch, s, d, way):
        return remote(
            block(ch, s, d), from_z.at[way, ch, s, d], zs.at[way, ch, s, d], zr.at[way, ch, s, d],
            index_at(z + 1 - 2 * way, y, core),
        )

    def compute(ch):
        load(ch).wait()
        for part in range(2):
            value = loaded[ch, part].astype(mask.dtype) * mask[...]
            natural[:, :, part * samples : (part + 1) * samples] = value
        pair = natural[...].reshape(inputs, 2 * samples).astype(jnp.bfloat16)
        pair = jnp.concatenate([pair, pair], axis=1)
        for turn in range(CORES):
            c = (core + 1 + turn) % CORES
            for yy in range(ny):
                for zz in range(nz):
                    left[yy * nz + zz] = natural[owned[index_at(zz, yy, c)]]
            part = left[...].reshape(inputs // CORES, 2 * samples).astype(jnp.bfloat16)
            other = jnp.concatenate([part[:, samples:], -part[:, :samples]], axis=1)
            dims = (((1,), (1,)), ((), ()))
            both = jnp.concatenate([part, other], axis=1)
            total = lax.dot_general(both, pair, dims, preferred_element_type=jnp.float32)
            gram[ch, c] = total.reshape(ny, nz, rows, inputs)
            if turn == 0:
                if isinstance(ch, int) and ch == 0:
                    amount = 1 + (ny > 1) + (z > 0).astype(jnp.int32) + (z < nz - 1).astype(jnp.int32)
                    pl.semaphore_wait(barrier, amount)
                core_copy(ch).start()

    def send_ends(at, ch, s, d):
        if d > 0:
            when(at == 0, lambda: z_copy(ch, s, d, 0).start())
        if d < nz - 1:
            when(at == nz - 1, lambda: z_copy(ch, s, d, 1).start())

    def begin(ch, is_wide):
        core_copy(ch).wait_recv()
        gram[ch, core] += from_core[ch]
        for d in far_first(nz):
            if ny > 1 and not is_wide:
                y_copy(ch, d).start()
            else:
                for s in range(ny):
                    send_ends(z, ch, s, d)

    def merge(at, ch, d):
        y_copy(ch, d).wait_recv()
        gram[ch, core, y, d] += from_y[ch, d]
        send_ends(at, ch, 0, d)

    def chain(at, ch, s, d, way):
        inside = at <= d if way == 0 else at >= d
        follows = at > 0 if way == 0 else at < nz - 1

        def act():
            z_copy(ch, s, d, way).wait_recv()
            into = block(ch, s, d)
            into[...] += from_z[way, ch, s, d]
            when(at != d, lambda: z_copy(ch, s, d, way).start())

        if isinstance(at, int):
            when(inside and follows, act)
        else:
            when(jnp.logical_and(inside, follows), act)

    def cross(at, ch):
        cross_copy(ch).start()

    def flag_copy(step):
        target = lax.rem(me + step, count)
        return remote(packed, gathered.at[me], gs.at[0], gr.at[0], target)

    def flags_all():
        whole = gathered.at[pl.ds(0, count - 1)]
        return remote(whole, whole, gs.at[0], gr.at[0], index_at(z, y, 1 - core))

    def keep_copy(ch):
        return pltpu.make_async_copy(gram.at[ch, core, y, z], kept.at[ch], ks.at[ch])

    def own_copy(ch):
        return pltpu.make_async_copy(turned.at[ch, me], mirrored.at[ch, me], os.at[ch])

    def mirror_copy(ch, step):
        target = lax.rem(me + step, count)
        return remote(turned.at[ch, target], mirrored.at[ch, me], fs.at[ch], fr.at[ch], target)

    def mirror_all(ch):
        whole = pl.ds(0, count - 1)
        return remote(turned.at[ch, whole], mirrored.at[ch, whole], fs.at[ch], fr.at[ch], index_at(z, y, 1 - core))

    def finish(at, ch):
        if ny > 1 and isinstance(ch, int) and ch in wide:
            cross_copy(ch).wait_recv()
            gram[ch, core, y, z] += from_y[ch, 0]
        keep_copy(ch).start()
        flipped = gram[ch, core, y, z].T
        each = rows // pack
        if each > 1:
            flipped = flipped.reshape(count, each, pack, rows)
            lane = lax.broadcasted_iota(jnp.int32, (count * pack, width), 1) // rows
            space = jnp.zeros((count * pack, width - rows), jnp.float32)
            total = None
            for a in range(each):
                piece = jnp.concatenate([flipped[:, a].reshape(count * pack, rows), space], axis=1)
                if a:
                    piece = pltpu.roll(piece, a * rows, 1)
                total = piece if total is None else jnp.where(lane == a, piece, total)
            flipped = total
        folded[...] = flipped.reshape(count, pack, width)
        for k in range(count):
            turned[ch, k] = folded[owned[k]]
        own_copy(ch).start()
        for step in range(1, count):
            mirror_copy(ch, step).start()

    def send_flags():
        for step in range(1, count):
            flag_copy(step).start()

    def make_scale():
        flags_all().wait_recv()
        for index in range(count):
            value = jnp.where(me == index, packed[...], gathered[index])
            words_all[index * subs : (index + 1) * subs, :] = value[:subs, :words]
        every = words_all[...]
        slots = count * subs
        broad = max(span, 128)
        lane = lax.broadcasted_iota(jnp.int32, (slots, broad), 1)
        columns = []
        for word in range(0, words, broad // span):
            value = jnp.broadcast_to(every[:, word : word + 1], (slots, broad))
            for extra in range(1, broad // span):
                value = jnp.where(lane >= extra * span, every[:, word + extra : word + extra + 1], value)
            bits = jnp.right_shift(value, (lane % span) // 2)
            columns.append(jnp.bitwise_and(bits, 1).astype(jnp.float32))
        good = jnp.concatenate(columns, axis=1).astype(jnp.bfloat16)
        counts = lax.dot_general(good, good, (((0,), (0,)), ((), ())), preferred_element_type=jnp.float32)
        pairs[...] = counts.reshape(count, rows, inputs)
        scale[...] = 0.5 / jnp.maximum(length * pairs[owned[me]], 1.0)

    def wait_sent(ch, s, d, way):
        z_copy(ch, s, d, way).wait_send()

    def finale(at):
        for ch in range(chans):
            core_copy(ch).wait_send()
            for d in range(nz):
                if ny > 1 and ch not in wide:
                    y_copy(ch, d).wait_send()
                for s in range(ny if ch in wide else 1):
                    when(at < d, functools.partial(wait_sent, ch, s, d, 0))
                    when(at > d, functools.partial(wait_sent, ch, s, d, 1))
            if ch in wide:
                cross_copy(ch).wait_send()
            mirror_all(ch).wait_send()
            keep_copy(ch).wait()
            own_copy(ch).wait()
        flags_all().wait_send()
        for ch in range(chans):
            mirror_all(ch).wait_recv()

    compute(0)

    def body(ch, carry):
        compute(ch)
        if ny == 1 or not wide:
            begin(ch - 1, False)
        else:
            special = functools.reduce(jnp.logical_or, [ch - 1 == one for one in wide])
            pl.when(special)(lambda: begin(ch - 1, True))
            pl.when(jnp.logical_not(special))(lambda: begin(ch - 1, False))
        return carry

    lax.fori_loop(1, chans, body, 0)
    begin(chans - 1, chans - 1 in wide)

    if nz <= STATIC:
        for at, events in enumerate(plan(nz, ny, chans, wide)):

            def play(at=at, events=events):
                acts = {"merge": merge, "chain": chain, "cross": cross, "finish": finish}
                done = 0
                for _, name, args in events:
                    acts[name](at, *args)
                    if name == "finish":
                        done += 1
                        if done == 1:
                            send_flags()
                make_scale()
                finale(at)

            pl.when(z == at)(play)
    else:

        def line(ch, carry):
            for d in far_first(nz) if ny > 1 else ():
                merge(z, ch, d)
            for i in range(nz):
                for way, d in ((0, nz - 1 - i), (1, i)):
                    chain(z, ch, 0, d, way)
            finish(z, ch)
            return carry

        lax.fori_loop(0, chans, line, 0)
        send_flags()
        make_scale()
        finale(z)


def assemble(owned, kept, mirrored, scale, out, holder):
    chans, count, pack, width = mirrored.shape
    rows, inputs = scale.shape
    each = rows // pack
    for k in range(count):
        holder[owned[k]] = k
    per = 128 // rows
    lane = lax.broadcasted_iota(jnp.int32, (pack, 128), 1) // rows
    factor = scale[...]
    for ch in range(chans):
        mirror = []
        for group in range(count // per):
            pieces = [mirrored[ch, holder[group * per + u]] for u in range(per)]
            if each == 1:
                total = None
                for u, piece in enumerate(pieces):
                    piece = jnp.concatenate([piece, jnp.zeros((rows, 128 - rows), piece.dtype)], axis=1)
                    piece = pltpu.roll(piece, u * rows, 1) if u else piece
                    total = piece if total is None else jnp.where(lane == u, piece, total)
                mirror.append(total)
                continue
            turns = []
            for shift in range(per):
                total = pieces[shift]
                for v in range(1, per):
                    total = jnp.where(lane == v, pieces[(v + shift) % per], total)
                turns.append(pltpu.roll(total, shift * rows, 1) if shift else total)
            parts = []
            for a in range(each):
                total = turns[-a % per]
                for u in range(1, per):
                    total = jnp.where(lane == u, turns[(u - a) % per], total)
                parts.append(total)
            mirror.append(jnp.concatenate(parts, axis=0))
        left = kept[ch]
        right = jnp.concatenate(mirror, axis=1)
        out[:, ch, 0, :] = (left + right) * factor
        out[:, ch, 1, :] = (left - right) * factor


def shards(nz, ny, voltages, antenna_flags, owned_tile):
    count = nz * ny * CORES
    chans, _, inputs, samples = voltages.shape
    rows = inputs // count
    wide = (1,) if ny > 1 and nz <= STATIC else ()
    held = jnp.bfloat16 if rows % 16 == 0 else jnp.float32
    each = max(1, 128 // rows)
    each = each if rows % (8 * each) == 0 else 1
    pack, width = rows // each, rows * each
    vmem = pl.BlockSpec(memory_space=pltpu.VMEM)
    smem = pl.BlockSpec(memory_space=pltpu.SMEM)
    hbm = pl.BlockSpec(memory_space=pltpu.HBM)
    dma = pltpu.SemaphoreType.DMA
    sizes = antenna_flags.shape
    slots = ny if wide else 1
    blocks = jax.ShapeDtypeStruct((chans, count, pack, width), jnp.float32)
    kept, mirrored, scale = pl.pallas_call(
        functools.partial(kernel, nz, ny, wide),
        out_shape=(
            jax.ShapeDtypeStruct((chans, rows, inputs), jnp.float32),
            blocks,
            jax.ShapeDtypeStruct((rows, inputs), jnp.float32),
        ),
        in_specs=[smem, smem, vmem, hbm],
        out_specs=(hbm, hbm, vmem),
        scratch_shapes=[
            pltpu.VMEM((chans, 2, count, rows, samples), voltages.dtype),
            pltpu.VMEM((count * sizes[0], sizes[1]), jnp.int32),
            pltpu.VMEM((count, rows, samples), held),
            pltpu.VMEM((count, rows, 2 * samples), held),
            pltpu.VMEM((count // CORES, rows, 2 * samples), held),
            pltpu.VMEM((chans, CORES, ny, nz, rows, inputs), jnp.float32),
            pltpu.VMEM((chans, ny, nz, rows, inputs), jnp.float32),
            pltpu.VMEM((chans, nz, rows, inputs), jnp.float32),
            pltpu.VMEM((2, chans, slots, nz, rows, inputs), jnp.float32),
            pltpu.VMEM(blocks.shape, jnp.float32),
            pltpu.VMEM(blocks.shape[1:], jnp.float32),
            pltpu.VMEM((count, rows, inputs), jnp.float32),
            pltpu.VMEM((count,) + sizes, jnp.int32),
            dma((chans,)), dma((chans,)), dma((chans,)), dma((chans, nz)), dma((chans, nz)),
            dma((2, chans, slots, nz)), dma((2, chans, slots, nz)), dma((chans,)), dma((chans,)),
            dma((1,)), dma((1,)), dma((chans,)), dma((chans,)),
        ],
        compiler_params=pltpu.CompilerParams(
            collective_id=0, has_side_effects=True, vmem_limit_bytes=60 * 1024 * 1024
        ),
    )(owned_tile, antenna_flags, antenna_flags, voltages.reshape(chans, 2, count, rows, samples))
    return pl.pallas_call(
        assemble,
        out_shape=jax.ShapeDtypeStruct((rows, chans, 2, inputs), jnp.float32),
        in_specs=[smem, vmem, vmem, vmem],
        out_specs=vmem,
        scratch_shapes=[pltpu.SMEM((count,), jnp.int32)],
    )(owned_tile, kept, mirrored, scale)


def solution(mesh):
    nz, ny = grid_of(mesh)
    return jax.shard_map(
        functools.partial(shards, nz, ny),
        mesh=mesh,
        in_specs=(P("band", None, None, "tm"), P("tm", "band"), P()),
        out_specs=P("tm", "band", None, None),
        check_vma=False,
    )
```

```python
import functools
import heapq

import jax
import jax.numpy as jnp
from jax import lax
from jax.experimental import pallas as pl
from jax.experimental.pallas import tpu as pltpu
from jax.sharding import PartitionSpec as P

MESH = pl.DeviceIdType.MESH
CORES = 2
BLOCK = 1.42
HOP = 2.0
FIRST = 4.0
START = 12.5
SLACK = 3.0
LATE = 7.0
STATIC = 4
HELD = 2
DIRECT = 2


def WIDE(nz):
    return {(1, d) for d in range(nz)}


def grid_of(mesh):
    count = mesh.shape["tm"]
    ny = 2 if mesh.shape["band"] < 4 and count % (4 * CORES) == 0 else 1
    return count // (ny * CORES), ny


def far_first(nz, z=None):
    middle = (nz - 1) / 2 if z is None else z
    return sorted(range(nz), key=lambda d: (-abs(d - middle), d))


def pick(z, values):
    if isinstance(z, int):
        return values[z]
    return sum(jnp.where(z == k, value, 0) for k, value in enumerate(values))


def when(condition, act):
    if isinstance(condition, bool):
        if condition:
            act()
    else:
        pl.when(condition)(act)


def plan(nz, ny, chans, wide, held, late):
    order = far_first(nz)
    mixed = sorted({ch for ch, _ in wide})
    events = [[] for _ in range(nz)]
    free = [[0.0, 0.0] for _ in range(nz)]
    queue, merged, landed, ended = [], set(), set(), {}
    sent = {}
    serial = iter(range(1 << 30))

    def add(time, *what):
        heapq.heappush(queue, (time if what[0] == "own" else max(time, START), next(serial), what))

    def note(z, time, name, *args):
        events[z].append((time, next(serial), name, args))

    def slack(ch):
        return SLACK if ch < chans - 2 else 0.0

    def forward(now, z, ch, s, d, way):
        free[z][way] = max(free[z][way], now) + BLOCK
        add(free[z][way] + HOP, "land", z + 1 - 2 * way, ch, s, d, way)

    def own(now, z, ch, s, d):
        merged.add((z, ch, s, d))
        if z == 0 and d > 0:
            forward(now, z, ch, s, d, 0)
        if z == nz - 1 and d < nz - 1:
            forward(now, z, ch, s, d, 1)
        for way in range(2):
            if (z, ch, s, d, way) in landed:
                join(now, z, ch, s, d, way)

    def join(now, z, ch, s, d, way):
        if z != d:
            note(z, now, "chain", ch, s, d, way)
            forward(now, z, ch, s, d, way)
            return
        note(z, now + slack(ch), "chain", ch, s, d, way)
        ended[z, ch, s] = ended.get((z, ch, s), 0) + 1
        if ended[z, ch, s] < (2 if 0 < z < nz - 1 else 1):
            return
        if s == 1:
            note(z, now + slack(ch), "cross", ch)
            pushes[z] = max(pushes[z], now + slack(ch))
            add(max(now, crossing) + BLOCK * len(mixed) + HOP, "whole", z, ch)
        else:
            add(now, "whole", z, ch)

    clock = FIRST
    crossing = 0.0
    pushes = [0.0] * nz
    for ch in range(chans):
        if ch == held:
            crossing = clock
            clock += BLOCK * len(mixed)
        steps = 0
        for z in range(nz):
            line = [d for d in far_first(nz, z) if (ch, d) not in wide and ny > 1]
            steps = len(line)
            for i, d in enumerate(line):
                add(clock + BLOCK * (i + 1) + HOP, "merge", z, ch, d)
            for d in order:
                if d not in line:
                    for s in range(ny):
                        add(FIRST + 1.5 * ch, "own", z, ch, s, d)
        clock += BLOCK * steps
    parts = {}
    while queue:
        now, _, (name, z, ch, *rest) = heapq.heappop(queue)
        if name == "merge":
            note(z, now, "merge", ch, *rest)
            own(now, z, ch, 0, *rest)
        elif name == "own":
            own(now, z, ch, *rest)
        elif name == "land":
            landed.add((z, ch, *rest))
            if (z, ch, *rest[:2]) in merged:
                join(now, z, ch, *rest)
        else:
            parts[z, ch] = parts.get((z, ch), 0) + 1
            if parts[z, ch] == (2 if (ch, z) in wide else 1):
                note(z, now + slack(ch), "finish", ch)
                last = now + slack(ch)
                if ch < late:
                    sent[z] = max(sent.get(z, 0.0), last)
                if 0 < z < nz - 1 or ch >= late:
                    for way, planes in ((0, nz - 1 - z), (1, z)):
                        free[z][way] = max(free[z][way], now) + BLOCK * planes / nz
    for z in range(nz):
        if late:
            note(z, max(sent.values()) + HOP, "relay")
            if z in (0, nz - 1):
                note(z, max(sent[z], clock + HOP + 0.1), "bulk")
        if ny > 1 and held < chans:
            note(z, pushes[z], "push")
        events[z].sort()
    return [[(name, args) for _, _, name, args in line] for line in events]


def kernel(nz, ny, wide, held, late, owned, flags, packed, volts, kept, mirrored, scale, loaded, words_all, mask, natural, left,
           gram, from_core, from_y, from_z, turned, folded, landed, factor, pairs, gathered,
           ls, cs, cr, ys, yr, zs, zr, fs, fr, ds, dr, bs, br, xs, gs, ts):
    count = nz * ny * CORES
    column = nz * CORES
    chans, _, tiles, rows, samples = volts.shape
    inputs = tiles * rows
    pack, width = folded.shape[1:]
    static = nz <= STATIC
    mixed = sorted({ch for ch, _ in wide})
    me = lax.axis_index("tm")
    core = lax.rem(me, CORES)
    y = lax.rem(me // CORES, ny)
    z = me // (CORES * ny)

    def index_at(zz, yy, cc):
        return (zz * ny + yy) * CORES + cc

    partner = index_at(z, y, 1 - core)
    opposite = index_at(z, 1 - y if ny > 1 else 0, core)
    barrier = pltpu.get_barrier_semaphore()

    def greet(target):
        pl.semaphore_signal(barrier, inc=1, device_id={"tm": target}, device_id_type=MESH)

    greet(partner)
    if ny > 1:
        greet(opposite)
    pl.when(z > 0)(lambda: greet(index_at(z - 1, y, core)))
    pl.when(z < nz - 1)(lambda: greet(index_at(z + 1, y, core)))

    def load(ch):
        return pltpu.make_async_copy(volts.at[ch], loaded.at[ch], ls.at[ch])

    for ch in range(chans):
        load(ch).start()

    subs, words = flags.shape
    length = samples // subs
    span = inputs // words
    shift = lax.broadcasted_iota(jnp.int32, (span, length), 0) // 2
    for word in range(words):
        for sub in range(subs):
            bits = jnp.right_shift(jnp.full((span, length), flags[sub, word], jnp.int32), shift)
            good = jnp.bitwise_and(bits, 1).astype(jnp.float32).astype(mask.dtype)
            good = good.reshape(span // rows, rows, length)
            mask[word * (span // rows) : (word + 1) * (span // rows), :, sub * length : (sub + 1) * length] = good

    def remote(src, dst, send, recv, target):
        return pltpu.make_async_remote_copy(
            src_ref=src, dst_ref=dst, send_sem=send, recv_sem=recv,
            device_id={"tm": target}, device_id_type=MESH,
        )

    def core_copy(ch):
        return remote(gram.at[ch, 1 - core], from_core.at[ch], cs.at[0], cr.at[ch], partner)

    def half_copy(ch, yy, slot):
        return remote(gram.at[ch, 1 - core, yy], from_core.at[ch, yy], cs.at[0], cr.at[slot], partner)

    def core_all():
        return remote(from_core, from_core, cs.at[0], cr.at[0], partner)

    def y_copy(ch, d):
        return remote(gram.at[ch, core, 1 - y, d], from_y.at[ch, d], ys.at[ch], yr.at[ch, d], opposite)

    def y_all(ch, blocks):
        part = from_y.at[ch, pl.ds(0, blocks)]
        return remote(part, part, ys.at[ch], yr.at[ch, 0], opposite)

    def block(ch, s, d):
        return gram.at[ch, core, lax.rem(y + s, ny) if ny > 1 else 0, d]

    def unit(ch, s):
        return chans + mixed.index(ch) if s else ch

    def z_copy(ch, s, d, way):
        u, slot = unit(ch, s), d + 1 - way
        return remote(
            block(ch, s, d), from_z.at[u, slot], zs.at[way, u, 0 if static else d], zr.at[u, slot],
            index_at(z + 1 - 2 * way, y, core),
        )

    def z_all(way, u, blocks):
        part = from_z.at[u, pl.ds(0, blocks)]
        return remote(part, part, zs.at[way, u, 0], zr.at[u, 0], partner)

    def prepare(ch, slot=0):
        load(ch).wait()
        for part in range(2):
            value = loaded[ch, part].astype(mask.dtype) * mask[...]
            natural[slot, :, :, part * samples : (part + 1) * samples] = value

    def multiply(ch, c, first, lines, slot=0):
        pair = natural[slot].reshape(inputs, 2 * samples).astype(jnp.bfloat16)
        pair = jnp.concatenate([pair, pair], axis=1)
        for yy in range(lines):
            for zz in range(nz):
                left[yy * nz + zz] = natural[slot, owned[index_at(zz, first + yy, c)]]
        part = left[0 : lines * nz].reshape(lines * nz * rows, 2 * samples).astype(jnp.bfloat16)
        other = jnp.concatenate([part[:, samples:], -part[:, :samples]], axis=1)
        dims = (((1,), (1,)), ((), ()))
        both = jnp.concatenate([part, other], axis=1)
        total = lax.dot_general(both, pair, dims, preferred_element_type=jnp.float32)
        if lines == ny:
            gram[ch, c] = total.reshape(ny, nz, rows, inputs)
        else:
            gram[ch, c, first] = total.reshape(nz, rows, inputs)

    def send_ends(at, ch, s, d):
        if d > 0:
            when(at == 0, lambda: z_copy(ch, s, d, 0).start())
        if d < nz - 1:
            when(at == nz - 1, lambda: z_copy(ch, s, d, 1).start())

    def issue(ch):
        known = isinstance(ch, int)
        if ny > 1 and (not known or ch < held):
            skip = [d for d in range(nz) if known and (ch, d) in wide]
            lines = [[d for d in far_first(nz, k) if d not in skip] for k in range(nz if static else 0)]
            for i in range(nz - len(skip)):
                y_copy(ch, pick(z, [line[i] for line in lines]) if static else i).start()
        for d in far_first(nz):
            if ny == 1 or (known and (ch, d) in wide):
                for s in range(ny):
                    send_ends(z, ch, s, d)

    def push(at):
        for ch in range(held, chans):
            for d in far_first(nz, at):
                if (ch, d) not in wide:
                    y_copy(ch, d).start()

    def begin(ch):
        core_copy(ch).wait_recv()
        gram[ch, core] += from_core[ch]
        if isinstance(ch, int) or not wide:
            issue(ch)
        else:
            for k in range(2, chans - 1):
                pl.when(ch == k)(functools.partial(issue, k))

    def merge(at, ch, d):
        y_copy(ch, d).wait_recv()
        gram[ch, core, y, d] += from_y[ch, d]
        send_ends(at, ch, 0, d)

    def chain(at, ch, s, d, way):
        inside = at <= d if way == 0 else at >= d
        follows = at > 0 if way == 0 else at < nz - 1

        def act():
            z_copy(ch, s, d, way).wait_recv()
            into = block(ch, s, d)
            into[...] += from_z[unit(ch, s), d + 1 - way]
            when(at != d, lambda: z_copy(ch, s, d, way).start())

        if isinstance(at, int):
            when(inside and follows, act)
        else:
            when(jnp.logical_and(inside, follows), act)

    def cross(at, ch):
        y_copy(ch, at).start()

    def others(yy_range):
        return [(dz, yy, dc) for dz in range(nz) for yy in yy_range for dc in range(CORES) if dz or yy or dc]

    def place(at, dz, dy, dc):
        zz = (at + dz) % nz if isinstance(at, int) else lax.rem(at + dz, nz)
        return zz, (lax.rem(y + dy, ny) if ny > 1 else 0), lax.rem(core + dc, CORES)

    def flag_copy(at, hop):
        target = index_at(*place(at, *hop))
        return remote(packed, gathered.at[me], gs.at[0], gs.at[1], target)

    def flags_all():
        whole = gathered.at[pl.ds(0, count - 1)]
        return remote(whole, whole, gs.at[0], gs.at[1], partner)

    def blocks_of(shape):
        return mirrored.at[pl.ds(0, shape[0]), 0, pl.ds(0, shape[1])]

    def passes(at, ch):
        return ny > 1 and static and isinstance(ch, int) and 0 < at < nz - 1 and ch < late

    def wait_bytes(shape, send, recv):
        part = blocks_of(shape)
        return remote(part, part, send, recv, partner)

    near_hops = others((0,))
    far_hops = [(dz, 1, dc) for dz in range(nz) for dc in range(CORES)] if ny > 1 else []
    mine = z * CORES + core
    inner = pl.ds(CORES, column - 2 * CORES)

    def near_copy(at, ch, hop):
        zz, yy, cc = place(at, *hop)
        return remote(
            turned.at[ch, zz * CORES + cc], landed.at[ch, :, mine - CORES], fs.at[0], fr.at[ch], index_at(zz, yy, cc)
        )

    def near_wait(at, ch):
        count_in = column - 2 * CORES - (0 < at < nz - 1)
        part = landed.at[ch, :, pl.ds(0, count_in)]
        return remote(part, part, fs.at[0], fr.at[ch], partner)

    def send_copy(at, ch, hop):
        zz, yy, cc = place(at, *hop)
        return remote(
            turned.at[ch, zz * CORES + cc, hop[1]], mirrored.at[ch, hop[1], mine], ds.at[ch - late], dr.at[ch - late],
            index_at(zz, yy, cc),
        )

    def bulk_copy(at, hop):
        zz, yy, cc = place(at, *hop)
        group = pl.ds(0, late)
        return remote(
            turned.at[group, zz * CORES + cc, hop[1]], mirrored.at[group, hop[1], mine], bs.at[hop[1]], br.at[hop[1]],
            index_at(zz, yy, cc),
        )

    def relay_copy(ch):
        return remote(landed.at[ch, 1], mirrored.at[ch, 1, inner], xs.at[0], xs.at[1], opposite)

    def relay_all():
        part = landed.at[:, 1]
        return remote(part, part, xs.at[0], xs.at[1], opposite)

    def near_out(ch):
        return pltpu.make_async_copy(landed.at[ch, 0], mirrored.at[ch, 0, inner], ts.at[1])

    def own_copy(ch):
        return pltpu.make_async_copy(turned.at[ch, mine, 0], mirrored.at[ch, 0, mine], ts.at[3])

    def keep_copy(ch):
        return pltpu.make_async_copy(gram.at[ch, core, y, z], kept.at[ch], ts.at[0])

    def scale_copy():
        return pltpu.make_async_copy(factor, scale, ts.at[2])

    def finish(at, ch):
        if isinstance(at, int) and (ch, at) in wide:
            y_copy(ch, at).wait_recv()
            gram[ch, core, y, at] += from_y[ch, at]
        keep_copy(ch).start()
        flipped = gram[ch, core, y, z].T
        each = rows // pack
        if each > 1:
            flipped = flipped.reshape(count, each, pack, rows)
            lane = lax.broadcasted_iota(jnp.int32, (count * pack, width), 1) // rows
            space = jnp.zeros((count * pack, width - rows), jnp.float32)
            total = None
            for a in range(each):
                piece = jnp.concatenate([flipped[:, a].reshape(count * pack, rows), space], axis=1)
                if a:
                    piece = pltpu.roll(piece, a * rows, 1)
                total = piece if total is None else jnp.where(lane == a, piece, total)
            flipped = total
        folded[...] = flipped.reshape(count, pack, width)
        for zz in range(nz):
            for cc in range(CORES):
                for dy in range(ny):
                    yy = lax.rem(y + dy, ny) if ny > 1 else 0
                    turned[ch, zz * CORES + cc, dy] = folded[owned[index_at(zz, yy, cc)]]
        if passes(at, ch):
            landed[ch, :, mine - CORES] = turned[ch, mine]
            for hop in near_hops:
                near_copy(at, ch, hop).start()
            return
        own_copy(ch).start()
        if not isinstance(ch, int) or ch >= late:
            hops = near_hops + far_hops
            if isinstance(at, int):
                hops.sort(key=lambda hop: (-abs((at + hop[0]) % nz - at), (at + hop[0]) % nz))
            for hop in hops:
                send_copy(at, ch, hop).start()

    def bulk(at):
        for hop in sorted(near_hops + far_hops, key=lambda hop: abs((at + hop[0]) % nz - at)):
            bulk_copy(at, hop).start()

    def relay(at):
        for ch in range(late):
            near_wait(at, ch).wait_recv()
            near_out(ch).start()
            relay_copy(ch).start()

    def send_flags(at):
        for hop in others(range(ny)):
            flag_copy(at, hop).start()

    def make_scale():
        flags_all().wait_recv()
        for index in range(count):
            value = jnp.where(me == index, packed[...], gathered[index])
            words_all[index * subs : (index + 1) * subs, :] = value[:subs, :words]
        every = words_all[...]
        slots = count * subs
        broad = max(span, 128)
        lane = lax.broadcasted_iota(jnp.int32, (slots, broad), 1)
        columns = []
        for word in range(0, words, broad // span):
            value = jnp.broadcast_to(every[:, word : word + 1], (slots, broad))
            for extra in range(1, broad // span):
                value = jnp.where(lane >= extra * span, every[:, word + extra : word + extra + 1], value)
            bits = jnp.right_shift(value, (lane % span) // 2)
            columns.append(jnp.bitwise_and(bits, 1).astype(jnp.float32))
        good = jnp.concatenate(columns, axis=1).astype(jnp.bfloat16)
        counts = lax.dot_general(good, good, (((0,), (0,)), ((), ())), preferred_element_type=jnp.float32)
        pairs[...] = counts.reshape(count, rows, inputs)
        factor[...] = 0.5 / jnp.maximum(length * pairs[owned[me]], 1.0)
        scale_copy().start()

    def wait_sent(ch, d, way):
        z_copy(ch, 0, d, way).wait_send()

    def finale(at):
        core_all().wait_send()
        for ch in range(chans):
            if ny > 1:
                y_all(ch, sum((ch, d) not in wide or d == at for d in range(nz))).wait_send()
            if static:
                for s in range(2 if ch in mixed else 1):
                    for way, line in ((0, range(at + 1, nz)), (1, range(at))):
                        blocks = sum(s == 0 or (ch, d) in wide for d in line)
                        if blocks:
                            z_all(way, unit(ch, s), blocks).wait_send()
            else:
                for d in range(nz):
                    when(at < d, functools.partial(wait_sent, ch, d, 0))
                    when(at > d, functools.partial(wait_sent, ch, d, 1))
        flags_all().wait_send()
        pltpu.make_async_copy(from_y.at[:, 0], kept, ts.at[0]).wait()
        scale_copy().wait()
        if late:
            side = column - 2 * CORES
            ends = 2 * CORES
            inside = 0 < at < nz - 1
            pltpu.make_async_copy(landed.at[:, 0], mirrored.at[pl.ds(0, late), 0, inner], ts.at[1]).wait()
            relay_all().wait()
            if inside:
                part = turned.at[pl.ds(0, late), pl.ds(0, column - 1)]
                remote(part, part, fs.at[0], fr.at[0], partner).wait_send()
            else:
                wait_bytes((late, column - 1), bs.at[0], br.at[0]).wait_send()
                wait_bytes((late, column), bs.at[1], br.at[1]).wait_send()
            wait_bytes((late, ends - (not inside)), bs.at[0], br.at[0]).wait_recv()
            wait_bytes((late, ends), bs.at[1], br.at[1]).wait_recv()
            owned_blocks = chans - late if inside else chans
        else:
            owned_blocks = chans
        pltpu.make_async_copy(turned.at[pl.ds(0, owned_blocks), 0, 0], mirrored.at[pl.ds(0, owned_blocks), 0, 0], ts.at[3]).wait()
        whole = pl.ds(0, count - 1)
        for ch in range(late, chans):
            remote(folded.at[whole], folded.at[whole], ds.at[ch - late], dr.at[ch - late], partner).wait()

    prepare(0)
    turns = [lax.rem(core + 1 + turn, CORES) for turn in range(CORES)]
    amount = 1 + (ny > 1) + (z > 0).astype(jnp.int32) + (z < nz - 1).astype(jnp.int32)
    if ny > 1:
        for slot, yy in ((0, 1 - y), (chans, y)):
            multiply(0, turns[0], yy, 1)
            if slot == 0:
                pl.semaphore_wait(barrier, amount)
            half_copy(0, yy, slot).start()
    else:
        multiply(0, turns[0], 0, ny)
        pl.semaphore_wait(barrier, amount)
        core_copy(0).start()
    prepare(1, 1)
    multiply(1, turns[0], 0, ny, 1)
    core_copy(1).start()
    multiply(0, turns[1], 0, ny)

    def compute(ch):
        prepare(ch)
        multiply(ch, turns[0], 0, ny)
        core_copy(ch).start()
        multiply(ch, turns[1], 0, ny)

    if ny > 1:
        for slot, yy in ((0, 1 - y), (chans, y)):
            half_copy(0, yy, slot).wait_recv()
            gram[0, core, yy] += from_core[0, yy]
            if slot == 0:
                issue(0)
    else:
        begin(0)
    multiply(1, turns[1], 0, ny, 1)
    begin(1)

    def body(ch, carry):
        compute(ch)
        pl.when(ch > 2)(lambda: begin(ch - 1))
        return carry

    lax.fori_loop(2, chans, body, 0)
    begin(chans - 1)

    if static:
        for at, events in enumerate(plan(nz, ny, chans, wide, held, late)):

            def play(at=at, events=events):
                acts = {"merge": merge, "chain": chain, "cross": cross, "finish": finish, "push": push, "relay": relay, "bulk": bulk}
                fresh = True
                for name, args in events:
                    acts[name](at, *args)
                    if name == "finish" and fresh:
                        fresh = False
                        send_flags(at)
                make_scale()
                finale(at)

            pl.when(z == at)(play)
    else:

        def line(ch, carry):
            for d in far_first(nz) if ny > 1 else ():
                merge(z, ch, d)
            for i in range(nz):
                for way, d in ((0, nz - 1 - i), (1, i)):
                    chain(z, ch, 0, d, way)
            finish(z, ch)
            return carry

        lax.fori_loop(0, chans, line, 0)
        send_flags(z)
        make_scale()
        finale(z)


def assemble(ny, owned, kept, mirrored, scale, out, holder):
    chans, sides, column, pack, width = mirrored.shape
    rows, inputs = scale.shape
    count = sides * column
    each = rows // pack
    y = lax.rem(lax.axis_index("tm") // CORES, ny)
    for k in range(count):
        plane, rest = divmod(k, ny * CORES)
        yy, cc = divmod(rest, CORES)
        side = lax.rem(y + yy, ny) if ny > 1 else 0
        holder[owned[k]] = side * column + plane * CORES + cc
    per = 128 // rows
    lane = lax.broadcasted_iota(jnp.int32, (pack, 128), 1) // rows
    factor = scale[...]
    for ch in range(chans):
        mirror = []
        for group in range(count // per):
            pieces = []
            for u in range(per):
                index = holder[group * per + u]
                pieces.append(mirrored[ch, index // column, lax.rem(index, column)])
            if each == 1:
                total = None
                for u, piece in enumerate(pieces):
                    piece = jnp.concatenate([piece, jnp.zeros((rows, 128 - rows), piece.dtype)], axis=1)
                    piece = pltpu.roll(piece, u * rows, 1) if u else piece
                    total = piece if total is None else jnp.where(lane == u, piece, total)
                mirror.append(total)
                continue
            turns = []
            for shift in range(per):
                total = pieces[shift]
                for v in range(1, per):
                    total = jnp.where(lane == v, pieces[(v + shift) % per], total)
                turns.append(pltpu.roll(total, shift * rows, 1) if shift else total)
            parts = []
            for a in range(each):
                total = turns[-a % per]
                for u in range(1, per):
                    total = jnp.where(lane == u, turns[(u - a) % per], total)
                parts.append(total)
            mirror.append(jnp.concatenate(parts, axis=0))
        left = kept[ch]
        right = jnp.concatenate(mirror, axis=1)
        out[:, ch, 0, :] = (left + right) * factor
        out[:, ch, 1, :] = (left - right) * factor


def shards(nz, ny, voltages, antenna_flags, owned_tile):
    count = nz * ny * CORES
    column = nz * CORES
    chans, _, inputs, samples = voltages.shape
    rows = inputs // count
    static = nz <= STATIC
    wide = frozenset((ch, d) for ch, d in WIDE(nz) if ch < chans) if ny > 1 and static else frozenset()
    held = chans - HELD if wide else chans
    late = chans - DIRECT if wide else 0
    extra = len({ch for ch, _ in wide})
    held_type = jnp.bfloat16 if rows % 16 == 0 else jnp.float32
    each = max(1, 128 // rows)
    each = each if rows % (8 * each) == 0 else 1
    pack, width = rows // each, rows * each
    vmem = pl.BlockSpec(memory_space=pltpu.VMEM)
    smem = pl.BlockSpec(memory_space=pltpu.SMEM)
    hbm = pl.BlockSpec(memory_space=pltpu.HBM)
    dma = pltpu.SemaphoreType.DMA
    sizes = antenna_flags.shape
    kept, mirrored, scale = pl.pallas_call(
        functools.partial(kernel, nz, ny, wide, held, late),
        out_shape=(
            jax.ShapeDtypeStruct((chans, rows, inputs), jnp.float32),
            jax.ShapeDtypeStruct((chans, ny, column, pack, width), jnp.float32),
            jax.ShapeDtypeStruct((rows, inputs), jnp.float32),
        ),
        in_specs=[smem, smem, vmem, hbm],
        out_specs=(hbm, hbm, hbm),
        scratch_shapes=[
            pltpu.VMEM((chans, 2, count, rows, samples), voltages.dtype),
            pltpu.VMEM((count * sizes[0], sizes[1]), jnp.int32),
            pltpu.VMEM((count, rows, samples), held_type),
            pltpu.VMEM((2, count, rows, 2 * samples), held_type),
            pltpu.VMEM((count // CORES, rows, 2 * samples), held_type),
            pltpu.VMEM((chans, CORES, ny, nz, rows, inputs), jnp.float32),
            pltpu.VMEM((chans, ny, nz, rows, inputs), jnp.float32),
            pltpu.VMEM((chans, nz, rows, inputs), jnp.float32),
            pltpu.VMEM((chans + extra, nz + 1, rows, inputs), jnp.float32),
            pltpu.VMEM((chans, column, ny, pack, width), jnp.float32),
            pltpu.VMEM((count, pack, width), jnp.float32),
            pltpu.VMEM((max(late, 1), ny, max(column - 2 * CORES, 1), pack, width), jnp.float32),
            pltpu.VMEM((rows, inputs), jnp.float32),
            pltpu.VMEM((count, rows, inputs), jnp.float32),
            pltpu.VMEM((count,) + sizes, jnp.int32),
            dma((chans,)), dma((1,)), dma((chans + 1,)), dma((chans,)), dma((chans, nz)),
            dma((2, chans + extra, 1 if static else nz)), dma((chans + extra, nz + 1)),
            dma((1,)), dma((max(late, 1),)), dma((chans - late,)), dma((chans - late,)), dma((2,)), dma((2,)), dma((2,)), dma((2,)), dma((4,)),
        ],
        compiler_params=pltpu.CompilerParams(
            collective_id=0, has_side_effects=True, vmem_limit_bytes=60 * 1024 * 1024
        ),
    )(owned_tile, antenna_flags, antenna_flags, voltages.reshape(chans, 2, count, rows, samples))
    return pl.pallas_call(
        functools.partial(assemble, ny),
        out_shape=jax.ShapeDtypeStruct((rows, chans, 2, inputs), jnp.float32),
        in_specs=[smem, vmem, vmem, vmem],
        out_specs=vmem,
        scratch_shapes=[pltpu.SMEM((count,), jnp.int32)],
    )(owned_tile, kept, mirrored, scale)


def solution(mesh):
    nz, ny = grid_of(mesh)
    return jax.shard_map(
        functools.partial(shards, nz, ny),
        mesh=mesh,
        in_specs=(P("band", None, None, "tm"), P("tm", "band"), P()),
        out_specs=P("tm", "band", None, None),
        check_vma=False,
    )
```

```python
import functools
import heapq

import jax
import jax.numpy as jnp
from jax import lax
from jax.experimental import pallas as pl
from jax.experimental.pallas import tpu as pltpu
from jax.sharding import PartitionSpec as P

MESH = pl.DeviceIdType.MESH
CORES = 2
BLOCK = 1.42
HOP = 2.0
FIRST = 4.0
START = 12.5
SLACK = 3.0
LATE = 7.0
STATIC = 4
HELD = 3
DIRECT = 3
EARLY = 3


def WIDE(nz):
    return {(1, d) for d in range(nz)}


def grid_of(mesh):
    count = mesh.shape["tm"]
    ny = 2 if mesh.shape["band"] < 4 and count % (4 * CORES) == 0 else 1
    return count // (ny * CORES), ny


def far_first(nz, z=None):
    middle = (nz - 1) / 2 if z is None else z
    return sorted(range(nz), key=lambda d: (-abs(d - middle), d))


def last_order(nz, z, channels):
    ranks = list(enumerate(far_first(nz, z)))
    return [(ch, d) for _, _, ch, d in sorted((i + ch, -ch, ch, d) for ch in channels for i, d in ranks)]


def pick(z, values):
    if isinstance(z, int):
        return values[z]
    return sum(jnp.where(z == k, value, 0) for k, value in enumerate(values))


def when(condition, act):
    if isinstance(condition, bool):
        if condition:
            act()
    else:
        pl.when(condition)(act)


def plan(nz, ny, chans, wide, held, early, late):
    order = far_first(nz)
    mixed = sorted({ch for ch, _ in wide})
    events = [[] for _ in range(nz)]
    free = [[0.0, 0.0] for _ in range(nz)]
    queue, merged, landed, ended = [], set(), set(), {}
    sent = {}
    serial = iter(range(1 << 30))

    def add(time, *what):
        heapq.heappush(queue, (time if what[0] == "own" else max(time, START), next(serial), what))

    def note(z, time, name, *args):
        events[z].append((time, next(serial), name, args))

    def slack(ch):
        return SLACK if ch < chans - 2 else 0.0

    def forward(now, z, ch, s, d, way):
        free[z][way] = max(free[z][way], now) + BLOCK
        add(free[z][way] + HOP, "land", z + 1 - 2 * way, ch, s, d, way)

    def own(now, z, ch, s, d):
        merged.add((z, ch, s, d))
        if z == 0 and d > 0:
            forward(now, z, ch, s, d, 0)
        if z == nz - 1 and d < nz - 1:
            forward(now, z, ch, s, d, 1)
        for way in range(2):
            if (z, ch, s, d, way) in landed:
                join(now, z, ch, s, d, way)

    def join(now, z, ch, s, d, way):
        if z != d:
            note(z, now, "chain", ch, s, d, way)
            forward(now, z, ch, s, d, way)
            return
        note(z, now + slack(ch), "chain", ch, s, d, way)
        ended[z, ch, s] = ended.get((z, ch, s), 0) + 1
        if ended[z, ch, s] < (2 if 0 < z < nz - 1 else 1):
            return
        if s == 1:
            note(z, now + slack(ch), "cross", ch)
            pushes[z] = max(pushes[z], now + slack(ch))
            add(max(now, crossing) + BLOCK * len(mixed) + HOP, "whole", z, ch)
        else:
            add(now, "whole", z, ch)

    clock = FIRST
    crossing = 0.0
    pushes = [0.0] * nz
    for ch in range(chans):
        if ch == held:
            crossing = clock
            clock += BLOCK * len(mixed)
            for z in range(nz):
                for i, (each, d) in enumerate(last_order(nz, z, range(held, chans))):
                    add(clock + BLOCK * (i + 1) + HOP, "merge", z, each, d)
            clock += BLOCK * nz * (chans - held)
            break
        steps = 0
        for z in range(nz):
            line = [d for d in far_first(nz, z) if (ch, d) not in wide and ny > 1]
            steps = len(line)
            for i, d in enumerate(line):
                add(clock + BLOCK * (i + 1) + HOP, "merge", z, ch, d)
            for d in order:
                if d not in line:
                    for s in range(ny):
                        add(FIRST + 1.5 * ch, "own", z, ch, s, d)
        clock += BLOCK * steps
    parts = {}
    while queue:
        now, _, (name, z, ch, *rest) = heapq.heappop(queue)
        if name == "merge":
            note(z, now, "merge", ch, *rest)
            own(now, z, ch, 0, *rest)
        elif name == "own":
            own(now, z, ch, *rest)
        elif name == "land":
            landed.add((z, ch, *rest))
            if (z, ch, *rest[:2]) in merged:
                join(now, z, ch, *rest)
        else:
            parts[z, ch] = parts.get((z, ch), 0) + 1
            if parts[z, ch] == (2 if (ch, z) in wide else 1):
                note(z, now + slack(ch), "finish", ch)
                last = now + slack(ch)
                if ch < late:
                    sent[z] = max(sent.get(z, 0.0), last)
                if 0 < z < nz - 1 or not early <= ch < late:
                    for way, planes in ((0, nz - 1 - z), (1, z)):
                        free[z][way] = max(free[z][way], now) + BLOCK * planes / nz
    for z in range(nz):
        if late:
            note(z, max(sent.values()) + HOP, "relay")
            if z in (0, nz - 1) and early < late:
                note(z, max(sent[z], clock + HOP + 0.1), "bulk")
        if ny > 1 and held < chans:
            note(z, pushes[z], "push")
        events[z].sort()
    return [[(name, args) for _, _, name, args in line] for line in events]


def kernel(nz, ny, wide, held, early, late, owned, flags, packed, volts, kept, mirrored, scale, loaded, words_all, mask, natural, left,
           gram, from_core, from_y, from_z, turned, folded, landed, factor, pairs, gathered,
           ls, cs, cr, ys, yr, zs, zr, fs, fr, ds, dr, bs, br, xs, xr, gs, ts):
    count = nz * ny * CORES
    column = nz * CORES
    chans, _, tiles, rows, samples = volts.shape
    inputs = tiles * rows
    pack, width = folded.shape[1:]
    static = nz <= STATIC
    mixed = sorted({ch for ch, _ in wide})
    me = lax.axis_index("tm")
    core = lax.rem(me, CORES)
    y = lax.rem(me // CORES, ny)
    z = me // (CORES * ny)

    def index_at(zz, yy, cc):
        return (zz * ny + yy) * CORES + cc

    partner = index_at(z, y, 1 - core)
    opposite = index_at(z, 1 - y if ny > 1 else 0, core)
    barrier = pltpu.get_barrier_semaphore()

    def greet(target):
        pl.semaphore_signal(barrier, inc=1, device_id={"tm": target}, device_id_type=MESH)

    greet(partner)
    if ny > 1:
        greet(opposite)
    pl.when(z > 0)(lambda: greet(index_at(z - 1, y, core)))
    pl.when(z < nz - 1)(lambda: greet(index_at(z + 1, y, core)))

    def load(ch):
        return pltpu.make_async_copy(volts.at[ch], loaded.at[ch], ls.at[ch])

    for ch in range(chans):
        load(ch).start()

    subs, words = flags.shape
    length = samples // subs
    span = inputs // words
    shift = lax.broadcasted_iota(jnp.int32, (span, length), 0) // 2
    for word in range(words):
        for sub in range(subs):
            bits = jnp.right_shift(jnp.full((span, length), flags[sub, word], jnp.int32), shift)
            good = jnp.bitwise_and(bits, 1).astype(jnp.float32).astype(mask.dtype)
            good = good.reshape(span // rows, rows, length)
            mask[word * (span // rows) : (word + 1) * (span // rows), :, sub * length : (sub + 1) * length] = good

    def remote(src, dst, send, recv, target):
        return pltpu.make_async_remote_copy(
            src_ref=src, dst_ref=dst, send_sem=send, recv_sem=recv,
            device_id={"tm": target}, device_id_type=MESH,
        )

    def core_copy(ch):
        return remote(gram.at[ch, 1 - core], from_core.at[ch], cs.at[0], cr.at[ch], partner)

    def half_copy(ch, yy, slot):
        return remote(gram.at[ch, 1 - core, yy], from_core.at[ch, yy], cs.at[0], cr.at[slot], partner)

    def core_all():
        return remote(from_core, from_core, cs.at[0], cr.at[0], partner)

    def y_copy(ch, d):
        return remote(gram.at[ch, core, 1 - y, d], from_y.at[ch, d], ys.at[ch], yr.at[ch, d], opposite)

    def y_all(ch, blocks):
        part = from_y.at[ch, pl.ds(0, blocks)]
        return remote(part, part, ys.at[ch], yr.at[ch, 0], opposite)

    def block(ch, s, d):
        return gram.at[ch, core, lax.rem(y + s, ny) if ny > 1 else 0, d]

    def unit(ch, s):
        return chans + mixed.index(ch) if s else ch

    def z_copy(ch, s, d, way):
        u, slot = unit(ch, s), d + 1 - way
        return remote(
            block(ch, s, d), from_z.at[u, slot], zs.at[way, u, 0 if static else d], zr.at[u, slot],
            index_at(z + 1 - 2 * way, y, core),
        )

    def z_all(way, u, blocks):
        part = from_z.at[u, pl.ds(0, blocks)]
        return remote(part, part, zs.at[way, u, 0], zr.at[u, 0], partner)

    def prepare(ch, slot=0):
        load(ch).wait()
        for part in range(2):
            value = loaded[ch, part].astype(mask.dtype) * mask[...]
            natural[slot, :, :, part * samples : (part + 1) * samples] = value

    def multiply(ch, c, first, lines, slot=0):
        pair = natural[slot].reshape(inputs, 2 * samples).astype(jnp.bfloat16)
        pair = jnp.concatenate([pair, pair], axis=1)
        for yy in range(lines):
            for zz in range(nz):
                left[yy * nz + zz] = natural[slot, owned[index_at(zz, first + yy, c)]]
        part = left[0 : lines * nz].reshape(lines * nz * rows, 2 * samples).astype(jnp.bfloat16)
        other = jnp.concatenate([part[:, samples:], -part[:, :samples]], axis=1)
        dims = (((1,), (1,)), ((), ()))
        both = jnp.concatenate([part, other], axis=1)
        total = lax.dot_general(both, pair, dims, preferred_element_type=jnp.float32)
        if lines == ny:
            gram[ch, c] = total.reshape(ny, nz, rows, inputs)
        else:
            gram[ch, c, first] = total.reshape(nz, rows, inputs)

    def send_ends(at, ch, s, d):
        if d > 0:
            when(at == 0, lambda: z_copy(ch, s, d, 0).start())
        if d < nz - 1:
            when(at == nz - 1, lambda: z_copy(ch, s, d, 1).start())

    def issue(ch):
        known = isinstance(ch, int)
        if ny > 1 and (not known or ch < held):
            skip = [d for d in range(nz) if known and (ch, d) in wide]
            lines = [[d for d in far_first(nz, k) if d not in skip] for k in range(nz if static else 0)]
            for i in range(nz - len(skip)):
                y_copy(ch, pick(z, [line[i] for line in lines]) if static else i).start()
        for d in far_first(nz):
            if ny == 1 or (known and (ch, d) in wide):
                for s in range(ny):
                    send_ends(z, ch, s, d)

    def push(at):
        for ch, d in last_order(nz, at, range(held, chans)):
            y_copy(ch, d).start()

    def begin(ch):
        core_copy(ch).wait_recv()
        gram[ch, core] += from_core[ch]
        if isinstance(ch, int) or not wide:
            issue(ch)
        else:
            for k in range(2, chans - 1):
                pl.when(ch == k)(functools.partial(issue, k))

    def merge(at, ch, d):
        y_copy(ch, d).wait_recv()
        gram[ch, core, y, d] += from_y[ch, d]
        send_ends(at, ch, 0, d)

    def chain(at, ch, s, d, way):
        inside = at <= d if way == 0 else at >= d
        follows = at > 0 if way == 0 else at < nz - 1

        def act():
            z_copy(ch, s, d, way).wait_recv()
            into = block(ch, s, d)
            into[...] += from_z[unit(ch, s), d + 1 - way]
            when(at != d, lambda: z_copy(ch, s, d, way).start())

        if isinstance(at, int):
            when(inside and follows, act)
        else:
            when(jnp.logical_and(inside, follows), act)

    def cross(at, ch):
        y_copy(ch, at).start()

    def others(yy_range):
        return [(dz, yy, dc) for dz in range(nz) for yy in yy_range for dc in range(CORES) if dz or yy or dc]

    def place(at, dz, dy, dc):
        zz = (at + dz) % nz if isinstance(at, int) else lax.rem(at + dz, nz)
        return zz, (lax.rem(y + dy, ny) if ny > 1 else 0), lax.rem(core + dc, CORES)

    def flag_copy(at, hop):
        target = index_at(*place(at, *hop))
        return remote(packed, gathered.at[me], gs.at[0], gs.at[1], target)

    def flags_all():
        whole = gathered.at[pl.ds(0, count - 1)]
        return remote(whole, whole, gs.at[0], gs.at[1], partner)

    def blocks_of(shape):
        return mirrored.at[pl.ds(0, shape[0]), 0, pl.ds(0, shape[1])]

    def passes(at, ch):
        return ny > 1 and static and isinstance(ch, int) and ch < (late if 0 < at < nz - 1 else early)

    def wait_bytes(shape, send, recv):
        part = blocks_of(shape)
        return remote(part, part, send, recv, partner)

    near_hops = others((0,))
    far_hops = [(dz, 1, dc) for dz in range(nz) for dc in range(CORES)] if ny > 1 else []
    mine = z * CORES + core
    inner = pl.ds(CORES, column - 2 * CORES)

    def near_copy(at, ch, hop):
        zz, yy, cc = place(at, *hop)
        return remote(
            turned.at[ch, zz * CORES + cc], landed.at[ch, :, mine], fs.at[0], fr.at[ch], index_at(zz, yy, cc)
        )

    def near_wait(at, ch):
        count_in = column - 1 if ch < early else column - 2 * CORES - (0 < at < nz - 1)
        part = landed.at[ch, :, pl.ds(0, count_in)]
        return remote(part, part, fs.at[0], fr.at[ch], partner)

    def send_copy(at, ch, hop):
        zz, yy, cc = place(at, *hop)
        return remote(
            turned.at[ch, zz * CORES + cc, hop[1]], mirrored.at[ch, hop[1], mine], ds.at[ch - late], dr.at[ch - late],
            index_at(zz, yy, cc),
        )

    def bulk_copy(at, hop):
        zz, yy, cc = place(at, *hop)
        group = pl.ds(early, late - early)
        return remote(
            turned.at[group, zz * CORES + cc, hop[1]], mirrored.at[group, hop[1], mine], bs.at[hop[1]], br.at[hop[1]],
            index_at(zz, yy, cc),
        )

    def slots(ch):
        return pl.ds(0, column) if ch < early else inner

    def relay_copy(ch):
        part = slots(ch)
        return remote(
            landed.at[ch, 1, part], mirrored.at[ch, 1, part], xs.at[int(ch < early)], xr.at[int(ch < early)], opposite
        )

    def relay_all(group, part, slot):
        chunk = landed.at[group, 1, part]
        return remote(chunk, chunk, xs.at[slot], xr.at[slot], opposite)

    def near_out(ch):
        part = slots(ch)
        return pltpu.make_async_copy(landed.at[ch, 0, part], mirrored.at[ch, 0, part], ts.at[1 + 3 * int(ch < early)])

    def near_out_all(group, part, slot):
        return pltpu.make_async_copy(landed.at[group, 0, part], mirrored.at[group, 0, part], ts.at[1 + 3 * slot])

    def own_copy(ch):
        return pltpu.make_async_copy(turned.at[ch, mine, 0], mirrored.at[ch, 0, mine], ts.at[3])

    def keep_copy(ch):
        return pltpu.make_async_copy(gram.at[ch, core, y, z], kept.at[ch], ts.at[0])

    def scale_copy():
        return pltpu.make_async_copy(factor, scale, ts.at[2])

    def finish(at, ch):
        if isinstance(at, int) and (ch, at) in wide:
            y_copy(ch, at).wait_recv()
            gram[ch, core, y, at] += from_y[ch, at]
        keep_copy(ch).start()
        flipped = gram[ch, core, y, z].T
        each = rows // pack
        if each > 1:
            flipped = flipped.reshape(count, each, pack, rows)
            lane = lax.broadcasted_iota(jnp.int32, (count * pack, width), 1) // rows
            space = jnp.zeros((count * pack, width - rows), jnp.float32)
            total = None
            for a in range(each):
                piece = jnp.concatenate([flipped[:, a].reshape(count * pack, rows), space], axis=1)
                if a:
                    piece = pltpu.roll(piece, a * rows, 1)
                total = piece if total is None else jnp.where(lane == a, piece, total)
            flipped = total
        folded[...] = flipped.reshape(count, pack, width)
        for zz in range(nz):
            for cc in range(CORES):
                for dy in range(ny):
                    yy = lax.rem(y + dy, ny) if ny > 1 else 0
                    turned[ch, zz * CORES + cc, dy] = folded[owned[index_at(zz, yy, cc)]]
        if passes(at, ch):
            landed[ch, :, mine] = turned[ch, mine]
            for hop in near_hops:
                near_copy(at, ch, hop).start()
            return
        own_copy(ch).start()
        if not isinstance(ch, int) or ch >= late:
            hops = near_hops + far_hops
            if isinstance(at, int):
                hops.sort(key=lambda hop: (-abs((at + hop[0]) % nz - at), (at + hop[0]) % nz))
            for hop in hops:
                send_copy(at, ch, hop).start()

    def bulk(at):
        for hop in sorted(near_hops + far_hops, key=lambda hop: abs((at + hop[0]) % nz - at)):
            bulk_copy(at, hop).start()

    def relay(at):
        for ch in range(late):
            near_wait(at, ch).wait_recv()
            near_out(ch).start()
            relay_copy(ch).start()

    def send_flags(at):
        for hop in others(range(ny)):
            flag_copy(at, hop).start()

    def make_scale():
        flags_all().wait_recv()
        for index in range(count):
            value = jnp.where(me == index, packed[...], gathered[index])
            words_all[index * subs : (index + 1) * subs, :] = value[:subs, :words]
        every = words_all[...]
        slots = count * subs
        broad = max(span, 128)
        lane = lax.broadcasted_iota(jnp.int32, (slots, broad), 1)
        columns = []
        for word in range(0, words, broad // span):
            value = jnp.broadcast_to(every[:, word : word + 1], (slots, broad))
            for extra in range(1, broad // span):
                value = jnp.where(lane >= extra * span, every[:, word + extra : word + extra + 1], value)
            bits = jnp.right_shift(value, (lane % span) // 2)
            columns.append(jnp.bitwise_and(bits, 1).astype(jnp.float32))
        good = jnp.concatenate(columns, axis=1).astype(jnp.bfloat16)
        counts = lax.dot_general(good, good, (((0,), (0,)), ((), ())), preferred_element_type=jnp.float32)
        pairs[...] = counts.reshape(count, rows, inputs)
        factor[...] = 0.5 / jnp.maximum(length * pairs[owned[me]], 1.0)
        scale_copy().start()

    def wait_sent(ch, d, way):
        z_copy(ch, 0, d, way).wait_send()

    def finale(at):
        core_all().wait_send()
        for ch in range(chans):
            if ny > 1:
                y_all(ch, sum((ch, d) not in wide or d == at for d in range(nz))).wait_send()
            if static:
                for s in range(2 if ch in mixed else 1):
                    for way, line in ((0, range(at + 1, nz)), (1, range(at))):
                        blocks = sum(s == 0 or (ch, d) in wide for d in line)
                        if blocks:
                            z_all(way, unit(ch, s), blocks).wait_send()
            else:
                for d in range(nz):
                    when(at < d, functools.partial(wait_sent, ch, d, 0))
                    when(at > d, functools.partial(wait_sent, ch, d, 1))
        flags_all().wait_send()
        pltpu.make_async_copy(from_y.at[:, 0], kept, ts.at[0]).wait()
        scale_copy().wait()
        if late:
            ends = 2 * CORES
            inside = 0 < at < nz - 1
            groups = [(pl.ds(early, late - early), inner, 0), (pl.ds(0, early), pl.ds(0, column), 1)]
            for group in groups:
                if group[0].size:
                    near_out_all(*group).wait()
                    relay_all(*group).wait()
            passed = late if inside else early
            if passed:
                part = turned.at[pl.ds(0, passed), pl.ds(0, column - 1)]
                remote(part, part, fs.at[0], fr.at[0], partner).wait_send()
            if early < late:
                if not inside:
                    wait_bytes((late - early, column - 1), bs.at[0], br.at[0]).wait_send()
                    wait_bytes((late - early, column), bs.at[1], br.at[1]).wait_send()
                wait_bytes((late - early, ends - (not inside)), bs.at[0], br.at[0]).wait_recv()
                wait_bytes((late - early, ends), bs.at[1], br.at[1]).wait_recv()
            owned_blocks = chans - passed
        else:
            owned_blocks = chans
        pltpu.make_async_copy(turned.at[pl.ds(0, owned_blocks), 0, 0], mirrored.at[pl.ds(0, owned_blocks), 0, 0], ts.at[3]).wait()
        whole = pl.ds(0, count - 1)
        for ch in range(late, chans):
            remote(folded.at[whole], folded.at[whole], ds.at[ch - late], dr.at[ch - late], partner).wait()

    prepare(0)
    turns = [lax.rem(core + 1 + turn, CORES) for turn in range(CORES)]
    amount = 1 + (ny > 1) + (z > 0).astype(jnp.int32) + (z < nz - 1).astype(jnp.int32)
    if ny > 1:
        for slot, yy in ((0, 1 - y), (chans, y)):
            multiply(0, turns[0], yy, 1)
            if slot == 0:
                pl.semaphore_wait(barrier, amount)
            half_copy(0, yy, slot).start()
    else:
        multiply(0, turns[0], 0, ny)
        pl.semaphore_wait(barrier, amount)
        core_copy(0).start()
    prepare(1, 1)
    multiply(1, turns[0], 0, ny, 1)
    core_copy(1).start()
    multiply(0, turns[1], 0, ny)

    def compute(ch):
        prepare(ch)
        multiply(ch, turns[0], 0, ny)
        core_copy(ch).start()
        multiply(ch, turns[1], 0, ny)

    if ny > 1:
        for slot, yy in ((0, 1 - y), (chans, y)):
            half_copy(0, yy, slot).wait_recv()
            gram[0, core, yy] += from_core[0, yy]
            if slot == 0:
                issue(0)
    else:
        begin(0)
    multiply(1, turns[1], 0, ny, 1)
    begin(1)

    def body(ch, carry):
        compute(ch)
        pl.when(ch > 2)(lambda: begin(ch - 1))
        return carry

    lax.fori_loop(2, chans, body, 0)
    begin(chans - 1)

    if static:
        for at, events in enumerate(plan(nz, ny, chans, wide, held, early, late)):

            def play(at=at, events=events):
                acts = {"merge": merge, "chain": chain, "cross": cross, "finish": finish, "push": push, "relay": relay, "bulk": bulk}
                fresh = True
                for name, args in events:
                    acts[name](at, *args)
                    if name == "finish" and fresh:
                        fresh = False
                        send_flags(at)
                make_scale()
                finale(at)

            pl.when(z == at)(play)
    else:

        def line(ch, carry):
            for d in far_first(nz) if ny > 1 else ():
                merge(z, ch, d)
            for i in range(nz):
                for way, d in ((0, nz - 1 - i), (1, i)):
                    chain(z, ch, 0, d, way)
            finish(z, ch)
            return carry

        lax.fori_loop(0, chans, line, 0)
        send_flags(z)
        make_scale()
        finale(z)


def assemble(ny, owned, kept, mirrored, scale, out, holder):
    chans, sides, column, pack, width = mirrored.shape
    rows, inputs = scale.shape
    count = sides * column
    each = rows // pack
    y = lax.rem(lax.axis_index("tm") // CORES, ny)
    for k in range(count):
        plane, rest = divmod(k, ny * CORES)
        yy, cc = divmod(rest, CORES)
        side = lax.rem(y + yy, ny) if ny > 1 else 0
        holder[owned[k]] = side * column + plane * CORES + cc
    per = 128 // rows
    lane = lax.broadcasted_iota(jnp.int32, (pack, 128), 1) // rows
    factor = scale[...]
    for ch in range(chans):
        mirror = []
        for group in range(count // per):
            pieces = []
            for u in range(per):
                index = holder[group * per + u]
                pieces.append(mirrored[ch, index // column, lax.rem(index, column)])
            if each == 1:
                total = None
                for u, piece in enumerate(pieces):
                    piece = jnp.concatenate([piece, jnp.zeros((rows, 128 - rows), piece.dtype)], axis=1)
                    piece = pltpu.roll(piece, u * rows, 1) if u else piece
                    total = piece if total is None else jnp.where(lane == u, piece, total)
                mirror.append(total)
                continue
            turns = []
            for shift in range(per):
                total = pieces[shift]
                for v in range(1, per):
                    total = jnp.where(lane == v, pieces[(v + shift) % per], total)
                turns.append(pltpu.roll(total, shift * rows, 1) if shift else total)
            parts = []
            for a in range(each):
                total = turns[-a % per]
                for u in range(1, per):
                    total = jnp.where(lane == u, turns[(u - a) % per], total)
                parts.append(total)
            mirror.append(jnp.concatenate(parts, axis=0))
        left = kept[ch]
        right = jnp.concatenate(mirror, axis=1)
        out[:, ch, 0, :] = (left + right) * factor
        out[:, ch, 1, :] = (left - right) * factor


def shards(nz, ny, voltages, antenna_flags, owned_tile):
    count = nz * ny * CORES
    column = nz * CORES
    chans, _, inputs, samples = voltages.shape
    rows = inputs // count
    static = nz <= STATIC
    wide = frozenset((ch, d) for ch, d in WIDE(nz) if ch < chans) if ny > 1 and static else frozenset()
    held = chans - HELD if wide else chans
    late = chans - DIRECT if wide else 0
    early = min(EARLY, late)
    extra = len({ch for ch, _ in wide})
    held_type = jnp.bfloat16 if rows % 16 == 0 else jnp.float32
    each = max(1, 128 // rows)
    each = each if rows % (8 * each) == 0 else 1
    pack, width = rows // each, rows * each
    vmem = pl.BlockSpec(memory_space=pltpu.VMEM)
    smem = pl.BlockSpec(memory_space=pltpu.SMEM)
    hbm = pl.BlockSpec(memory_space=pltpu.HBM)
    dma = pltpu.SemaphoreType.DMA
    sizes = antenna_flags.shape
    kept, mirrored, scale = pl.pallas_call(
        functools.partial(kernel, nz, ny, wide, held, early, late),
        out_shape=(
            jax.ShapeDtypeStruct((chans, rows, inputs), jnp.float32),
            jax.ShapeDtypeStruct((chans, ny, column, pack, width), jnp.float32),
            jax.ShapeDtypeStruct((rows, inputs), jnp.float32),
        ),
        in_specs=[smem, smem, vmem, hbm],
        out_specs=(hbm, hbm, hbm),
        scratch_shapes=[
            pltpu.VMEM((chans, 2, count, rows, samples), voltages.dtype),
            pltpu.VMEM((count * sizes[0], sizes[1]), jnp.int32),
            pltpu.VMEM((count, rows, samples), held_type),
            pltpu.VMEM((2, count, rows, 2 * samples), held_type),
            pltpu.VMEM((count // CORES, rows, 2 * samples), held_type),
            pltpu.VMEM((chans, CORES, ny, nz, rows, inputs), jnp.float32),
            pltpu.VMEM((chans, ny, nz, rows, inputs), jnp.float32),
            pltpu.VMEM((chans, nz, rows, inputs), jnp.float32),
            pltpu.VMEM((chans + extra, nz + 1, rows, inputs), jnp.float32),
            pltpu.VMEM((chans, column, ny, pack, width), jnp.float32),
            pltpu.VMEM((count, pack, width), jnp.float32),
            pltpu.VMEM((max(late, 1), ny, column, pack, width), jnp.float32),
            pltpu.VMEM((rows, inputs), jnp.float32),
            pltpu.VMEM((count, rows, inputs), jnp.float32),
            pltpu.VMEM((count,) + sizes, jnp.int32),
            dma((chans,)), dma((1,)), dma((chans + 1,)), dma((chans,)), dma((chans, nz)),
            dma((2, chans + extra, 1 if static else nz)), dma((chans + extra, nz + 1)),
            dma((1,)), dma((max(late, 1),)), dma((chans - late,)), dma((chans - late,)), dma((2,)), dma((2,)), dma((2,)), dma((2,)), dma((2,)), dma((5,)),
        ],
        compiler_params=pltpu.CompilerParams(
            collective_id=0, has_side_effects=True, vmem_limit_bytes=60 * 1024 * 1024
        ),
    )(owned_tile, antenna_flags, antenna_flags, voltages.reshape(chans, 2, count, rows, samples))
    return pl.pallas_call(
        functools.partial(assemble, ny),
        out_shape=jax.ShapeDtypeStruct((rows, chans, 2, inputs), jnp.float32),
        in_specs=[smem, vmem, vmem, vmem],
        out_specs=vmem,
        scratch_shapes=[pltpu.SMEM((count,), jnp.int32)],
    )(owned_tile, kept, mirrored, scale)


def solution(mesh):
    nz, ny = grid_of(mesh)
    return jax.shard_map(
        functools.partial(shards, nz, ny),
        mesh=mesh,
        in_specs=(P("band", None, None, "tm"), P("tm", "band"), P()),
        out_specs=P("tm", "band", None, None),
        check_vma=False,
    )
```

```python
import functools
import heapq

import jax
import jax.numpy as jnp
from jax import lax
from jax.experimental import pallas as pl
from jax.experimental.pallas import tpu as pltpu
from jax.sharding import PartitionSpec as P

MESH = pl.DeviceIdType.MESH
CORES = 2
BLOCK = 1.42
HOP = 2.0
FIRST = 4.0
START = 12.5
SLACK = 3.0
LATE = 7.0
STATIC = 4
HELD = 3
DIRECT = 3
EARLY = 3


def WIDE(nz):
    return {(1, d) for d in range(nz)}


def grid_of(mesh):
    count = mesh.shape["tm"]
    ny = 2 if mesh.shape["band"] < 4 and count % (4 * CORES) == 0 else 1
    return count // (ny * CORES), ny


def far_first(nz, z=None):
    middle = (nz - 1) / 2 if z is None else z
    return sorted(range(nz), key=lambda d: (-abs(d - middle), d))


def last_order(nz, z, channels):
    ranks = list(enumerate(far_first(nz, z)))
    return [(ch, d) for _, _, ch, d in sorted((i + ch, -ch, ch, d) for ch in channels for i, d in ranks)]


def pick(z, values):
    if isinstance(z, int):
        return values[z]
    return sum(jnp.where(z == k, value, 0) for k, value in enumerate(values))


def when(condition, act):
    if isinstance(condition, bool):
        if condition:
            act()
    else:
        pl.when(condition)(act)


def plan(nz, ny, chans, wide, held, early, late):
    order = far_first(nz)
    mixed = sorted({ch for ch, _ in wide})
    events = [[] for _ in range(nz)]
    free = [[0.0, 0.0] for _ in range(nz)]
    queue, merged, landed, ended = [], set(), set(), {}
    sent = {}
    serial = iter(range(1 << 30))

    def add(time, *what):
        heapq.heappush(queue, (time if what[0] == "own" else max(time, START), next(serial), what))

    def note(z, time, name, *args):
        events[z].append((time, next(serial), name, args))

    def slack(ch):
        return SLACK if ch < chans - 2 else 0.0

    def forward(now, z, ch, s, d, way):
        free[z][way] = max(free[z][way], now) + BLOCK
        add(free[z][way] + HOP, "land", z + 1 - 2 * way, ch, s, d, way)

    def own(now, z, ch, s, d):
        merged.add((z, ch, s, d))
        if z == 0 and d > 0:
            forward(now, z, ch, s, d, 0)
        if z == nz - 1 and d < nz - 1:
            forward(now, z, ch, s, d, 1)
        for way in range(2):
            if (z, ch, s, d, way) in landed:
                join(now, z, ch, s, d, way)

    def join(now, z, ch, s, d, way):
        if z != d:
            note(z, now, "chain", ch, s, d, way)
            forward(now, z, ch, s, d, way)
            return
        note(z, now + slack(ch), "chain", ch, s, d, way)
        ended[z, ch, s] = ended.get((z, ch, s), 0) + 1
        if ended[z, ch, s] < (2 if 0 < z < nz - 1 else 1):
            return
        if s == 1:
            note(z, now + slack(ch), "cross", ch)
            pushes[z] = max(pushes[z], now + slack(ch))
            add(max(now, crossing) + BLOCK * len(mixed) + HOP, "whole", z, ch)
        else:
            add(now, "whole", z, ch)

    clock = FIRST
    crossing = 0.0
    pushes = [0.0] * nz
    for ch in range(chans):
        if ch == held:
            crossing = clock
            clock += BLOCK * len(mixed)
            for z in range(nz):
                for i, (each, d) in enumerate(last_order(nz, z, range(held, chans))):
                    add(clock + BLOCK * (i + 1) + HOP, "merge", z, each, d)
            clock += BLOCK * nz * (chans - held)
            break
        steps = 0
        for z in range(nz):
            line = [d for d in far_first(nz, z) if (ch, d) not in wide and ny > 1]
            steps = len(line)
            for i, d in enumerate(line):
                add(clock + BLOCK * (i + 1) + HOP, "merge", z, ch, d)
            for d in order:
                if d not in line:
                    for s in range(ny):
                        add(FIRST + 1.5 * ch, "own", z, ch, s, d)
        clock += BLOCK * steps
    parts = {}
    while queue:
        now, _, (name, z, ch, *rest) = heapq.heappop(queue)
        if name == "merge":
            note(z, now, "merge", ch, *rest)
            own(now, z, ch, 0, *rest)
        elif name == "own":
            own(now, z, ch, *rest)
        elif name == "land":
            landed.add((z, ch, *rest))
            if (z, ch, *rest[:2]) in merged:
                join(now, z, ch, *rest)
        else:
            parts[z, ch] = parts.get((z, ch), 0) + 1
            if parts[z, ch] == (2 if (ch, z) in wide else 1):
                note(z, now + slack(ch), "finish", ch)
                last = now + slack(ch)
                if ch < late:
                    sent[z] = max(sent.get(z, 0.0), last)
                if 0 < z < nz - 1 or not early <= ch < late:
                    for way, planes in ((0, nz - 1 - z), (1, z)):
                        free[z][way] = max(free[z][way], now) + BLOCK * planes / nz
    for z in range(nz):
        if late:
            note(z, max(sent.values()) + HOP, "relay")
            if z in (0, nz - 1) and early < late:
                note(z, max(sent[z], clock + HOP + 0.1), "bulk")
        if ny > 1 and held < chans:
            note(z, pushes[z], "push")
        events[z].sort()
    return [[(name, args) for _, _, name, args in line] for line in events]


def kernel(nz, ny, wide, held, early, late, owned_in, flags_in, volts, kept, mirrored, scale, owned, flags, packed, loaded, words_all, mask, natural, left,
           gram, from_core, from_y, from_z, turned, folded, landed, factor, pairs, gathered,
           ls, cs, cr, ys, yr, zs, zr, fs, fr, ds, dr, bs, br, xs, xr, gs, ts, hs):
    count = nz * ny * CORES
    column = nz * CORES
    chans, _, tiles, rows, samples = volts.shape
    inputs = tiles * rows
    pack, width = folded.shape[1:]
    static = nz <= STATIC
    mixed = sorted({ch for ch, _ in wide})
    me = lax.axis_index("tm")
    core = lax.rem(me, CORES)
    y = lax.rem(me // CORES, ny)
    z = me // (CORES * ny)

    def index_at(zz, yy, cc):
        return (zz * ny + yy) * CORES + cc

    partner = index_at(z, y, 1 - core)
    opposite = index_at(z, 1 - y if ny > 1 else 0, core)
    barrier = pltpu.get_barrier_semaphore()

    def greet(target):
        pl.semaphore_signal(barrier, inc=1, device_id={"tm": target}, device_id_type=MESH)

    greet(partner)
    if ny > 1:
        greet(opposite)
    pl.when(z > 0)(lambda: greet(index_at(z - 1, y, core)))
    pl.when(z < nz - 1)(lambda: greet(index_at(z + 1, y, core)))

    def load(ch):
        return pltpu.make_async_copy(volts.at[ch], loaded.at[ch], ls.at[ch])

    small = [
        pltpu.make_async_copy(flags_in, flags, hs.at[0]),
        pltpu.make_async_copy(owned_in, owned, hs.at[1]),
        pltpu.make_async_copy(flags_in, packed, hs.at[2]),
    ]
    for copy in small:
        copy.start()
    load(0).start()
    for copy in small:
        copy.wait()
    for ch in range(1, chans):
        load(ch).start()

    subs, words = flags.shape
    length = samples // subs
    span = inputs // words
    shift = lax.broadcasted_iota(jnp.int32, (span, length), 0) // 2
    for word in range(words):
        for sub in range(subs):
            bits = jnp.right_shift(jnp.full((span, length), flags[sub, word], jnp.int32), shift)
            good = jnp.bitwise_and(bits, 1).astype(jnp.float32).astype(mask.dtype)
            good = good.reshape(span // rows, rows, length)
            mask[word * (span // rows) : (word + 1) * (span // rows), :, sub * length : (sub + 1) * length] = good

    def remote(src, dst, send, recv, target):
        return pltpu.make_async_remote_copy(
            src_ref=src, dst_ref=dst, send_sem=send, recv_sem=recv,
            device_id={"tm": target}, device_id_type=MESH,
        )

    def core_copy(ch):
        return remote(gram.at[ch, 1 - core], from_core.at[ch], cs.at[0], cr.at[ch], partner)

    def half_copy(ch, yy, slot):
        return remote(gram.at[ch, 1 - core, yy], from_core.at[ch, yy], cs.at[0], cr.at[slot], partner)

    def core_all():
        return remote(from_core, from_core, cs.at[0], cr.at[0], partner)

    def y_copy(ch, d):
        return remote(gram.at[ch, core, 1 - y, d], from_y.at[ch, d], ys.at[ch], yr.at[ch, d], opposite)

    def y_all(ch, blocks):
        part = from_y.at[ch, pl.ds(0, blocks)]
        return remote(part, part, ys.at[ch], yr.at[ch, 0], opposite)

    def block(ch, s, d):
        return gram.at[ch, core, lax.rem(y + s, ny) if ny > 1 else 0, d]

    def unit(ch, s):
        return chans + mixed.index(ch) if s else ch

    def z_copy(ch, s, d, way):
        u, slot = unit(ch, s), d + 1 - way
        return remote(
            block(ch, s, d), from_z.at[u, slot], zs.at[way, u, 0 if static else d], zr.at[u, slot],
            index_at(z + 1 - 2 * way, y, core),
        )

    def z_all(way, u, blocks):
        part = from_z.at[u, pl.ds(0, blocks)]
        return remote(part, part, zs.at[way, u, 0], zr.at[u, 0], partner)

    def prepare(ch, slot=0):
        load(ch).wait()
        for part in range(2):
            value = loaded[ch, part].astype(mask.dtype) * mask[...]
            natural[slot, :, :, part * samples : (part + 1) * samples] = value

    def multiply(ch, c, first, lines, slot=0):
        pair = natural[slot].reshape(inputs, 2 * samples).astype(jnp.bfloat16)
        pair = jnp.concatenate([pair, pair], axis=1)
        for yy in range(lines):
            for zz in range(nz):
                left[yy * nz + zz] = natural[slot, owned[index_at(zz, first + yy, c)]]
        part = left[0 : lines * nz].reshape(lines * nz * rows, 2 * samples).astype(jnp.bfloat16)
        other = jnp.concatenate([part[:, samples:], -part[:, :samples]], axis=1)
        dims = (((1,), (1,)), ((), ()))
        both = jnp.concatenate([part, other], axis=1)
        total = lax.dot_general(both, pair, dims, preferred_element_type=jnp.float32)
        if lines == ny:
            gram[ch, c] = total.reshape(ny, nz, rows, inputs)
        else:
            gram[ch, c, first] = total.reshape(nz, rows, inputs)

    def send_ends(at, ch, s, d):
        if d > 0:
            when(at == 0, lambda: z_copy(ch, s, d, 0).start())
        if d < nz - 1:
            when(at == nz - 1, lambda: z_copy(ch, s, d, 1).start())

    def issue(ch):
        known = isinstance(ch, int)
        if ny > 1 and (not known or ch < held):
            skip = [d for d in range(nz) if known and (ch, d) in wide]
            lines = [[d for d in far_first(nz, k) if d not in skip] for k in range(nz if static else 0)]
            for i in range(nz - len(skip)):
                y_copy(ch, pick(z, [line[i] for line in lines]) if static else i).start()
        for d in far_first(nz):
            if ny == 1 or (known and (ch, d) in wide):
                for s in range(ny):
                    send_ends(z, ch, s, d)

    def push(at):
        for ch, d in last_order(nz, at, range(held, chans)):
            y_copy(ch, d).start()

    def begin(ch):
        core_copy(ch).wait_recv()
        gram[ch, core] += from_core[ch]
        if isinstance(ch, int) or not wide:
            issue(ch)
        else:
            for k in range(2, chans - 1):
                pl.when(ch == k)(functools.partial(issue, k))

    def merge(at, ch, d):
        y_copy(ch, d).wait_recv()
        gram[ch, core, y, d] += from_y[ch, d]
        send_ends(at, ch, 0, d)

    def chain(at, ch, s, d, way):
        inside = at <= d if way == 0 else at >= d
        follows = at > 0 if way == 0 else at < nz - 1

        def act():
            z_copy(ch, s, d, way).wait_recv()
            into = block(ch, s, d)
            into[...] += from_z[unit(ch, s), d + 1 - way]
            when(at != d, lambda: z_copy(ch, s, d, way).start())

        if isinstance(at, int):
            when(inside and follows, act)
        else:
            when(jnp.logical_and(inside, follows), act)

    def cross(at, ch):
        y_copy(ch, at).start()

    def others(yy_range):
        return [(dz, yy, dc) for dz in range(nz) for yy in yy_range for dc in range(CORES) if dz or yy or dc]

    def place(at, dz, dy, dc):
        zz = (at + dz) % nz if isinstance(at, int) else lax.rem(at + dz, nz)
        return zz, (lax.rem(y + dy, ny) if ny > 1 else 0), lax.rem(core + dc, CORES)

    def flag_copy(at, hop):
        target = index_at(*place(at, *hop))
        return remote(packed, gathered.at[me], gs.at[0], gs.at[1], target)

    def flags_all():
        whole = gathered.at[pl.ds(0, count - 1)]
        return remote(whole, whole, gs.at[0], gs.at[1], partner)

    def blocks_of(shape):
        return mirrored.at[pl.ds(0, shape[0]), 0, pl.ds(0, shape[1])]

    def passes(at, ch):
        return ny > 1 and static and isinstance(ch, int) and ch < (late if 0 < at < nz - 1 else early)

    def wait_bytes(shape, send, recv):
        part = blocks_of(shape)
        return remote(part, part, send, recv, partner)

    near_hops = others((0,))
    far_hops = [(dz, 1, dc) for dz in range(nz) for dc in range(CORES)] if ny > 1 else []
    mine = z * CORES + core
    inner = pl.ds(CORES, column - 2 * CORES)

    def near_copy(at, ch, hop):
        zz, yy, cc = place(at, *hop)
        return remote(
            turned.at[ch, zz * CORES + cc], landed.at[ch, :, mine], fs.at[0], fr.at[ch], index_at(zz, yy, cc)
        )

    def near_wait(at, ch):
        count_in = column - 1 if ch < early else column - 2 * CORES - (0 < at < nz - 1)
        part = landed.at[ch, :, pl.ds(0, count_in)]
        return remote(part, part, fs.at[0], fr.at[ch], partner)

    def send_copy(at, ch, hop):
        zz, yy, cc = place(at, *hop)
        return remote(
            turned.at[ch, zz * CORES + cc, hop[1]], mirrored.at[ch, hop[1], mine], ds.at[ch - late], dr.at[ch - late],
            index_at(zz, yy, cc),
        )

    def bulk_copy(at, hop):
        zz, yy, cc = place(at, *hop)
        group = pl.ds(early, late - early)
        return remote(
            turned.at[group, zz * CORES + cc, hop[1]], mirrored.at[group, hop[1], mine], bs.at[hop[1]], br.at[hop[1]],
            index_at(zz, yy, cc),
        )

    def slots(ch):
        return pl.ds(0, column) if ch < early else inner

    def relay_copy(ch):
        part = slots(ch)
        return remote(
            landed.at[ch, 1, part], mirrored.at[ch, 1, part], xs.at[int(ch < early)], xr.at[int(ch < early)], opposite
        )

    def relay_all(group, part, slot):
        chunk = landed.at[group, 1, part]
        return remote(chunk, chunk, xs.at[slot], xr.at[slot], opposite)

    def near_out(ch):
        part = slots(ch)
        return pltpu.make_async_copy(landed.at[ch, 0, part], mirrored.at[ch, 0, part], ts.at[1 + 3 * int(ch < early)])

    def near_out_all(group, part, slot):
        return pltpu.make_async_copy(landed.at[group, 0, part], mirrored.at[group, 0, part], ts.at[1 + 3 * slot])

    def own_copy(ch):
        return pltpu.make_async_copy(turned.at[ch, mine, 0], mirrored.at[ch, 0, mine], ts.at[3])

    def keep_copy(ch):
        return pltpu.make_async_copy(gram.at[ch, core, y, z], kept.at[ch], ts.at[0])

    def scale_copy():
        return pltpu.make_async_copy(factor, scale, ts.at[2])

    def finish(at, ch):
        if isinstance(at, int) and (ch, at) in wide:
            y_copy(ch, at).wait_recv()
            gram[ch, core, y, at] += from_y[ch, at]
        keep_copy(ch).start()
        flipped = gram[ch, core, y, z].T
        each = rows // pack
        if each > 1:
            flipped = flipped.reshape(count, each, pack, rows)
            lane = lax.broadcasted_iota(jnp.int32, (count * pack, width), 1) // rows
            space = jnp.zeros((count * pack, width - rows), jnp.float32)
            total = None
            for a in range(each):
                piece = jnp.concatenate([flipped[:, a].reshape(count * pack, rows), space], axis=1)
                if a:
                    piece = pltpu.roll(piece, a * rows, 1)
                total = piece if total is None else jnp.where(lane == a, piece, total)
            flipped = total
        folded[...] = flipped.reshape(count, pack, width)
        for zz in range(nz):
            for cc in range(CORES):
                for dy in range(ny):
                    yy = lax.rem(y + dy, ny) if ny > 1 else 0
                    turned[ch, zz * CORES + cc, dy] = folded[owned[index_at(zz, yy, cc)]]
        if passes(at, ch):
            landed[ch, :, mine] = turned[ch, mine]
            for hop in near_hops:
                near_copy(at, ch, hop).start()
            return
        own_copy(ch).start()
        if not isinstance(ch, int) or ch >= late:
            hops = near_hops + far_hops
            if isinstance(at, int):
                hops.sort(key=lambda hop: (-abs((at + hop[0]) % nz - at), (at + hop[0]) % nz))
            for hop in hops:
                send_copy(at, ch, hop).start()

    def bulk(at):
        for hop in sorted(near_hops + far_hops, key=lambda hop: abs((at + hop[0]) % nz - at)):
            bulk_copy(at, hop).start()

    def relay(at):
        for ch in range(late):
            near_wait(at, ch).wait_recv()
            near_out(ch).start()
            relay_copy(ch).start()

    def send_flags(at):
        for hop in others(range(ny)):
            flag_copy(at, hop).start()

    def make_scale():
        flags_all().wait_recv()
        for index in range(count):
            value = jnp.where(me == index, packed[...], gathered[index])
            words_all[index * subs : (index + 1) * subs, :] = value[:subs, :words]
        every = words_all[...]
        slots = count * subs
        broad = max(span, 128)
        lane = lax.broadcasted_iota(jnp.int32, (slots, broad), 1)
        columns = []
        for word in range(0, words, broad // span):
            value = jnp.broadcast_to(every[:, word : word + 1], (slots, broad))
            for extra in range(1, broad // span):
                value = jnp.where(lane >= extra * span, every[:, word + extra : word + extra + 1], value)
            bits = jnp.right_shift(value, (lane % span) // 2)
            columns.append(jnp.bitwise_and(bits, 1).astype(jnp.float32))
        good = jnp.concatenate(columns, axis=1).astype(jnp.bfloat16)
        counts = lax.dot_general(good, good, (((0,), (0,)), ((), ())), preferred_element_type=jnp.float32)
        pairs[...] = counts.reshape(count, rows, inputs)
        factor[...] = 0.5 / jnp.maximum(length * pairs[owned[me]], 1.0)
        scale_copy().start()

    def wait_sent(ch, d, way):
        z_copy(ch, 0, d, way).wait_send()

    def finale(at):
        core_all().wait_send()
        for ch in range(chans):
            if ny > 1:
                y_all(ch, sum((ch, d) not in wide or d == at for d in range(nz))).wait_send()
            if static:
                for s in range(2 if ch in mixed else 1):
                    for way, line in ((0, range(at + 1, nz)), (1, range(at))):
                        blocks = sum(s == 0 or (ch, d) in wide for d in line)
                        if blocks:
                            z_all(way, unit(ch, s), blocks).wait_send()
            else:
                for d in range(nz):
                    when(at < d, functools.partial(wait_sent, ch, d, 0))
                    when(at > d, functools.partial(wait_sent, ch, d, 1))
        flags_all().wait_send()
        pltpu.make_async_copy(from_y.at[:, 0], kept, ts.at[0]).wait()
        scale_copy().wait()
        if late:
            ends = 2 * CORES
            inside = 0 < at < nz - 1
            groups = [(pl.ds(early, late - early), inner, 0), (pl.ds(0, early), pl.ds(0, column), 1)]
            for group in groups:
                if group[0].size:
                    near_out_all(*group).wait()
                    relay_all(*group).wait()
            passed = late if inside else early
            if passed:
                part = turned.at[pl.ds(0, passed), pl.ds(0, column - 1)]
                remote(part, part, fs.at[0], fr.at[0], partner).wait_send()
            if early < late:
                if not inside:
                    wait_bytes((late - early, column - 1), bs.at[0], br.at[0]).wait_send()
                    wait_bytes((late - early, column), bs.at[1], br.at[1]).wait_send()
                wait_bytes((late - early, ends - (not inside)), bs.at[0], br.at[0]).wait_recv()
                wait_bytes((late - early, ends), bs.at[1], br.at[1]).wait_recv()
            owned_blocks = chans - passed
        else:
            owned_blocks = chans
        pltpu.make_async_copy(turned.at[pl.ds(0, owned_blocks), 0, 0], mirrored.at[pl.ds(0, owned_blocks), 0, 0], ts.at[3]).wait()
        whole = pl.ds(0, count - 1)
        for ch in range(late, chans):
            remote(folded.at[whole], folded.at[whole], ds.at[ch - late], dr.at[ch - late], partner).wait()

    prepare(0)
    turns = [lax.rem(core + 1 + turn, CORES) for turn in range(CORES)]
    amount = 1 + (ny > 1) + (z > 0).astype(jnp.int32) + (z < nz - 1).astype(jnp.int32)
    if ny > 1:
        for slot, yy in ((0, 1 - y), (chans, y)):
            multiply(0, turns[0], yy, 1)
            if slot == 0:
                pl.semaphore_wait(barrier, amount)
            half_copy(0, yy, slot).start()
    else:
        multiply(0, turns[0], 0, ny)
        pl.semaphore_wait(barrier, amount)
        core_copy(0).start()
    prepare(1, 1)
    multiply(1, turns[0], 0, ny, 1)
    core_copy(1).start()
    multiply(0, turns[1], 0, ny)

    def compute(ch):
        prepare(ch)
        multiply(ch, turns[0], 0, ny)
        core_copy(ch).start()
        multiply(ch, turns[1], 0, ny)

    if ny > 1:
        for slot, yy in ((0, 1 - y), (chans, y)):
            half_copy(0, yy, slot).wait_recv()
            gram[0, core, yy] += from_core[0, yy]
            if slot == 0:
                issue(0)
    else:
        begin(0)
    multiply(1, turns[1], 0, ny, 1)
    begin(1)

    def body(ch, carry):
        compute(ch)
        pl.when(ch > 2)(lambda: begin(ch - 1))
        return carry

    lax.fori_loop(2, chans, body, 0)
    begin(chans - 1)

    if static:
        for at, events in enumerate(plan(nz, ny, chans, wide, held, early, late)):

            def play(at=at, events=events):
                acts = {"merge": merge, "chain": chain, "cross": cross, "finish": finish, "push": push, "relay": relay, "bulk": bulk}
                fresh = True
                for name, args in events:
                    acts[name](at, *args)
                    if name == "finish" and fresh:
                        fresh = False
                        send_flags(at)
                make_scale()
                finale(at)

            pl.when(z == at)(play)
    else:

        def line(ch, carry):
            for d in far_first(nz) if ny > 1 else ():
                merge(z, ch, d)
            for i in range(nz):
                for way, d in ((0, nz - 1 - i), (1, i)):
                    chain(z, ch, 0, d, way)
            finish(z, ch)
            return carry

        lax.fori_loop(0, chans, line, 0)
        send_flags(z)
        make_scale()
        finale(z)


def assemble(ny, step, owned_in, kept, mirrored, scale, out, owned, own, other, factors, result, holder, os, ms, rs, fs):
    chans, count, pack, width = mirrored.shape
    rows, inputs = scale.shape
    column = count // ny
    each = rows // pack
    y = lax.rem(lax.axis_index("tm") // CORES, ny)

    def fetch(part):
        group = pl.ds(part * step, step)
        return (
            pltpu.make_async_copy(mirrored.at[group], other.at[group], ms.at[part]),
            pltpu.make_async_copy(kept.at[group], own.at[group], os.at[part]),
        )

    scale_copy = pltpu.make_async_copy(scale, factors, fs.at[0])
    owned_copy = pltpu.make_async_copy(owned_in, owned, fs.at[1])
    owned_copy.start()
    scale_copy.start()
    for part in range(chans // step):
        for copy in fetch(part):
            copy.start()
    owned_copy.wait()
    for k in range(count):
        plane, rest = divmod(k, ny * CORES)
        yy, cc = divmod(rest, CORES)
        side = lax.rem(y + yy, ny) if ny > 1 else 0
        holder[owned[k]] = side * column + plane * CORES + cc
    per = 128 // rows
    lane = lax.broadcasted_iota(jnp.int32, (pack, 128), 1) // rows
    scale_copy.wait()
    factor = factors[...]
    for ch in range(chans):
        if ch % step == 0:
            for copy in fetch(ch // step):
                copy.wait()
        mirror = []
        for group in range(count // per):
            pieces = []
            for u in range(per):
                index = holder[group * per + u]
                pieces.append(other[ch, index])
            if each == 1:
                total = None
                for u, piece in enumerate(pieces):
                    piece = jnp.concatenate([piece, jnp.zeros((rows, 128 - rows), piece.dtype)], axis=1)
                    piece = pltpu.roll(piece, u * rows, 1) if u else piece
                    total = piece if total is None else jnp.where(lane == u, piece, total)
                mirror.append(total)
                continue
            turns = []
            for shift in range(per):
                total = pieces[shift]
                for v in range(1, per):
                    total = jnp.where(lane == v, pieces[(v + shift) % per], total)
                turns.append(pltpu.roll(total, shift * rows, 1) if shift else total)
            parts = []
            for a in range(each):
                total = turns[-a % per]
                for u in range(1, per):
                    total = jnp.where(lane == u, turns[(u - a) % per], total)
                parts.append(total)
            mirror.append(jnp.concatenate(parts, axis=0))
        left = own[ch]
        right = jnp.concatenate(mirror, axis=1)
        result[:, ch, 0, :] = (left + right) * factor
        result[:, ch, 1, :] = (left - right) * factor
        if ch % step == step - 1:
            group = pl.ds(ch + 1 - step, step)
            pltpu.make_async_copy(result.at[:, group], out.at[:, group], rs.at[0]).start()
    pltpu.make_async_copy(result, out, rs.at[0]).wait()


def shards(nz, ny, voltages, antenna_flags, owned_tile):
    count = nz * ny * CORES
    column = nz * CORES
    chans, _, inputs, samples = voltages.shape
    rows = inputs // count
    static = nz <= STATIC
    wide = frozenset((ch, d) for ch, d in WIDE(nz) if ch < chans) if ny > 1 and static else frozenset()
    held = chans - HELD if wide else chans
    late = chans - DIRECT if wide else 0
    early = min(EARLY, late)
    extra = len({ch for ch, _ in wide})
    held_type = jnp.bfloat16 if rows % 16 == 0 else jnp.float32
    each = max(1, 128 // rows)
    each = each if rows % (8 * each) == 0 else 1
    pack, width = rows // each, rows * each
    vmem = pl.BlockSpec(memory_space=pltpu.VMEM)
    smem = pl.BlockSpec(memory_space=pltpu.SMEM)
    hbm = pl.BlockSpec(memory_space=pltpu.HBM)
    dma = pltpu.SemaphoreType.DMA
    sizes = antenna_flags.shape
    kept, mirrored, scale = pl.pallas_call(
        functools.partial(kernel, nz, ny, wide, held, early, late),
        out_shape=(
            jax.ShapeDtypeStruct((chans, rows, inputs), jnp.float32),
            jax.ShapeDtypeStruct((chans, ny, column, pack, width), jnp.float32),
            jax.ShapeDtypeStruct((rows, inputs), jnp.float32),
        ),
        in_specs=[hbm, hbm, hbm],
        out_specs=(hbm, hbm, hbm),
        scratch_shapes=[
            pltpu.SMEM(owned_tile.shape, jnp.int32),
            pltpu.SMEM(sizes, jnp.int32),
            pltpu.VMEM(sizes, jnp.int32),
            pltpu.VMEM((chans, 2, count, rows, samples), voltages.dtype),
            pltpu.VMEM((count * sizes[0], sizes[1]), jnp.int32),
            pltpu.VMEM((count, rows, samples), held_type),
            pltpu.VMEM((2, count, rows, 2 * samples), held_type),
            pltpu.VMEM((count // CORES, rows, 2 * samples), held_type),
            pltpu.VMEM((chans, CORES, ny, nz, rows, inputs), jnp.float32),
            pltpu.VMEM((chans, ny, nz, rows, inputs), jnp.float32),
            pltpu.VMEM((chans, nz, rows, inputs), jnp.float32),
            pltpu.VMEM((chans + extra, nz + 1, rows, inputs), jnp.float32),
            pltpu.VMEM((chans, column, ny, pack, width), jnp.float32),
            pltpu.VMEM((count, pack, width), jnp.float32),
            pltpu.VMEM((max(late, 1), ny, column, pack, width), jnp.float32),
            pltpu.VMEM((rows, inputs), jnp.float32),
            pltpu.VMEM((count, rows, inputs), jnp.float32),
            pltpu.VMEM((count,) + sizes, jnp.int32),
            dma((chans,)), dma((1,)), dma((chans + 1,)), dma((chans,)), dma((chans, nz)),
            dma((2, chans + extra, 1 if static else nz)), dma((chans + extra, nz + 1)),
            dma((1,)), dma((max(late, 1),)), dma((chans - late,)), dma((chans - late,)), dma((2,)), dma((2,)), dma((2,)), dma((2,)), dma((2,)), dma((5,)), dma((3,)),
        ],
        compiler_params=pltpu.CompilerParams(
            collective_id=0, has_side_effects=True, vmem_limit_bytes=60 * 1024 * 1024
        ),
    )(owned_tile, antenna_flags, voltages.reshape(chans, 2, count, rows, samples))
    step = 2 if chans % 2 == 0 else 1
    return pl.pallas_call(
        functools.partial(assemble, ny, step),
        out_shape=jax.ShapeDtypeStruct((rows, chans, 2, inputs), jnp.float32),
        in_specs=[hbm, hbm, hbm, hbm],
        out_specs=hbm,
        scratch_shapes=[
            pltpu.SMEM((count,), jnp.int32),
            pltpu.VMEM((chans, rows, inputs), jnp.float32),
            pltpu.VMEM((chans, count, pack, width), jnp.float32),
            pltpu.VMEM((rows, inputs), jnp.float32),
            pltpu.VMEM((rows, chans, 2, inputs), jnp.float32),
            pltpu.SMEM((count,), jnp.int32),
            dma((chans // step,)), dma((chans // step,)), dma((1,)), dma((2,)),
        ],
    )(owned_tile, kept, mirrored.reshape(chans, count, pack, width), scale)


def solution(mesh):
    nz, ny = grid_of(mesh)
    return jax.shard_map(
        functools.partial(shards, nz, ny),
        mesh=mesh,
        in_specs=(P("band", None, None, "tm"), P("tm", "band"), P()),
        out_specs=P("tm", "band", None, None),
        check_vma=False,
    )
```

```python
import functools
import heapq

import jax
import jax.numpy as jnp
from jax import lax
from jax.experimental import pallas as pl
from jax.experimental.pallas import tpu as pltpu
from jax.sharding import PartitionSpec as P

MESH = pl.DeviceIdType.MESH
CORES = 2
BLOCK = 1.42
HOP = 2.0
FIRST = 4.0
START = 12.5
SLACK = 3.0
LATE = 7.0
STATIC = 4
HELD = 3
DIRECT = 3
EARLY = 3


def WIDE(nz):
    return {(1, d) for d in range(nz)}


def grid_of(mesh):
    count = mesh.shape["tm"]
    ny = 2 if mesh.shape["band"] < 4 and count % (4 * CORES) == 0 else 1
    return count // (ny * CORES), ny


def far_first(nz, z=None):
    middle = (nz - 1) / 2 if z is None else z
    return sorted(range(nz), key=lambda d: (-abs(d - middle), d))


def last_order(nz, z, channels):
    ranks = list(enumerate(far_first(nz, z)))
    return [(ch, d) for _, _, ch, d in sorted((i + ch, -ch, ch, d) for ch in channels for i, d in ranks)]


def pick(z, values):
    if isinstance(z, int):
        return values[z]
    return sum(jnp.where(z == k, value, 0) for k, value in enumerate(values))


def when(condition, act):
    if isinstance(condition, bool):
        if condition:
            act()
    else:
        pl.when(condition)(act)


def plan(nz, ny, chans, wide, held, early, late):
    order = far_first(nz)
    mixed = sorted({ch for ch, _ in wide})
    events = [[] for _ in range(nz)]
    free = [[0.0, 0.0] for _ in range(nz)]
    queue, merged, landed, ended = [], set(), set(), {}
    sent = {}
    serial = iter(range(1 << 30))

    def add(time, *what):
        heapq.heappush(queue, (time if what[0] == "own" else max(time, START), next(serial), what))

    def note(z, time, name, *args):
        events[z].append((time, next(serial), name, args))

    def slack(ch):
        return SLACK if ch < chans - 2 else 0.0

    def forward(now, z, ch, s, d, way):
        free[z][way] = max(free[z][way], now) + BLOCK
        add(free[z][way] + HOP, "land", z + 1 - 2 * way, ch, s, d, way)

    def own(now, z, ch, s, d):
        merged.add((z, ch, s, d))
        if z == 0 and d > 0:
            forward(now, z, ch, s, d, 0)
        if z == nz - 1 and d < nz - 1:
            forward(now, z, ch, s, d, 1)
        for way in range(2):
            if (z, ch, s, d, way) in landed:
                join(now, z, ch, s, d, way)

    def join(now, z, ch, s, d, way):
        if z != d:
            note(z, now, "chain", ch, s, d, way)
            forward(now, z, ch, s, d, way)
            return
        note(z, now + slack(ch), "chain", ch, s, d, way)
        ended[z, ch, s] = ended.get((z, ch, s), 0) + 1
        if ended[z, ch, s] < (2 if 0 < z < nz - 1 else 1):
            return
        if s == 1:
            note(z, now + slack(ch), "cross", ch)
            pushes[z] = max(pushes[z], now + slack(ch))
            add(max(now, crossing) + BLOCK * len(mixed) + HOP, "whole", z, ch)
        else:
            add(now, "whole", z, ch)

    clock = FIRST
    crossing = 0.0
    pushes = [0.0] * nz
    for ch in range(chans):
        if ch == held:
            crossing = clock
            clock += BLOCK * len(mixed)
            for z in range(nz):
                for i, (each, d) in enumerate(last_order(nz, z, range(held, chans))):
                    add(clock + BLOCK * (i + 1) + HOP, "merge", z, each, d)
            clock += BLOCK * nz * (chans - held)
            break
        steps = 0
        for z in range(nz):
            line = [d for d in far_first(nz, z) if (ch, d) not in wide and ny > 1]
            steps = len(line)
            for i, d in enumerate(line):
                add(clock + BLOCK * (i + 1) + HOP, "merge", z, ch, d)
            for d in order:
                if d not in line:
                    for s in range(ny):
                        add(FIRST + 1.5 * ch, "own", z, ch, s, d)
        clock += BLOCK * steps
    parts = {}
    while queue:
        now, _, (name, z, ch, *rest) = heapq.heappop(queue)
        if name == "merge":
            note(z, now, "merge", ch, *rest)
            own(now, z, ch, 0, *rest)
        elif name == "own":
            own(now, z, ch, *rest)
        elif name == "land":
            landed.add((z, ch, *rest))
            if (z, ch, *rest[:2]) in merged:
                join(now, z, ch, *rest)
        else:
            parts[z, ch] = parts.get((z, ch), 0) + 1
            if parts[z, ch] == (2 if (ch, z) in wide else 1):
                note(z, now + slack(ch), "finish", ch)
                last = now + slack(ch)
                if ch < late:
                    sent[z] = max(sent.get(z, 0.0), last)
                if 0 < z < nz - 1 or not early <= ch < late:
                    for way, planes in ((0, nz - 1 - z), (1, z)):
                        free[z][way] = max(free[z][way], now) + BLOCK * planes / nz
    for z in range(nz):
        if late:
            note(z, max(max(sent.values()), clock) + HOP + 0.05, "relay")
            if z in (0, nz - 1) and early < late:
                note(z, max(sent[z], clock - 1.0), "bulk")
        if ny > 1 and held < chans:
            note(z, pushes[z], "push")
        events[z].sort()
    return [[(name, args) for _, _, name, args in line] for line in events]


def kernel(nz, ny, wide, held, early, late, owned_in, flags_in, volts, kept, mirrored, scale, owned, flags, packed, loaded, words_all, mask, natural, left,
           gram, from_core, from_y, from_z, turned, folded, landed, factor, pairs, gathered,
           ls, cs, cr, ys, yr, zs, zr, fs, fr, ds, dr, bs, br, xs, xr, gs, ts, hs):
    count = nz * ny * CORES
    column = nz * CORES
    chans, _, tiles, rows, samples = volts.shape
    inputs = tiles * rows
    pack, width = folded.shape[1:]
    static = nz <= STATIC
    mixed = sorted({ch for ch, _ in wide})
    me = lax.axis_index("tm")
    core = lax.rem(me, CORES)
    y = lax.rem(me // CORES, ny)
    z = me // (CORES * ny)

    def index_at(zz, yy, cc):
        return (zz * ny + yy) * CORES + cc

    partner = index_at(z, y, 1 - core)
    opposite = index_at(z, 1 - y if ny > 1 else 0, core)
    barrier = pltpu.get_barrier_semaphore()

    def greet(target):
        pl.semaphore_signal(barrier, inc=1, device_id={"tm": target}, device_id_type=MESH)

    greet(partner)
    if ny > 1:
        greet(opposite)
    pl.when(z > 0)(lambda: greet(index_at(z - 1, y, core)))
    pl.when(z < nz - 1)(lambda: greet(index_at(z + 1, y, core)))

    def load(ch):
        return pltpu.make_async_copy(volts.at[ch], loaded.at[ch], ls.at[ch])

    small = [
        pltpu.make_async_copy(flags_in, flags, hs.at[0]),
        pltpu.make_async_copy(owned_in, owned, hs.at[1]),
        pltpu.make_async_copy(flags_in, packed, hs.at[2]),
    ]
    for copy in small:
        copy.start()
    load(0).start()
    for copy in small:
        copy.wait()
    for ch in range(1, chans):
        load(ch).start()

    subs, words = flags.shape
    length = samples // subs
    span = inputs // words
    shift = lax.broadcasted_iota(jnp.int32, (span, length), 0) // 2
    for word in range(words):
        for sub in range(subs):
            bits = jnp.right_shift(jnp.full((span, length), flags[sub, word], jnp.int32), shift)
            good = jnp.bitwise_and(bits, 1).astype(jnp.float32).astype(mask.dtype)
            good = good.reshape(span // rows, rows, length)
            mask[word * (span // rows) : (word + 1) * (span // rows), :, sub * length : (sub + 1) * length] = good

    def remote(src, dst, send, recv, target):
        return pltpu.make_async_remote_copy(
            src_ref=src, dst_ref=dst, send_sem=send, recv_sem=recv,
            device_id={"tm": target}, device_id_type=MESH,
        )

    def core_copy(ch):
        return remote(gram.at[ch, 1 - core], from_core.at[ch], cs.at[0], cr.at[ch], partner)

    def half_copy(ch, yy, slot):
        return remote(gram.at[ch, 1 - core, yy], from_core.at[ch, yy], cs.at[0], cr.at[slot], partner)

    def core_all():
        return remote(from_core, from_core, cs.at[0], cr.at[0], partner)

    def y_copy(ch, d):
        return remote(gram.at[ch, core, 1 - y, d], from_y.at[ch, d], ys.at[ch], yr.at[ch, d], opposite)

    def y_all(ch, blocks):
        part = from_y.at[ch, pl.ds(0, blocks)]
        return remote(part, part, ys.at[ch], yr.at[ch, 0], opposite)

    def block(ch, s, d):
        return gram.at[ch, core, lax.rem(y + s, ny) if ny > 1 else 0, d]

    def unit(ch, s):
        return chans + mixed.index(ch) if s else ch

    def z_copy(ch, s, d, way):
        u, slot = unit(ch, s), d + 1 - way
        return remote(
            block(ch, s, d), from_z.at[u, slot], zs.at[way, u, 0 if static else d], zr.at[u, slot],
            index_at(z + 1 - 2 * way, y, core),
        )

    def z_all(way, u, blocks):
        part = from_z.at[u, pl.ds(0, blocks)]
        return remote(part, part, zs.at[way, u, 0], zr.at[u, 0], partner)

    def prepare(ch, slot=0):
        load(ch).wait()
        for part in range(2):
            value = loaded[ch, part].astype(mask.dtype) * mask[...]
            natural[slot, :, :, part * samples : (part + 1) * samples] = value

    def multiply(ch, c, first, lines, slot=0):
        pair = natural[slot].reshape(inputs, 2 * samples).astype(jnp.bfloat16)
        pair = jnp.concatenate([pair, pair], axis=1)
        for yy in range(lines):
            for zz in range(nz):
                left[yy * nz + zz] = natural[slot, owned[index_at(zz, first + yy, c)]]
        part = left[0 : lines * nz].reshape(lines * nz * rows, 2 * samples).astype(jnp.bfloat16)
        other = jnp.concatenate([part[:, samples:], -part[:, :samples]], axis=1)
        dims = (((1,), (1,)), ((), ()))
        both = jnp.concatenate([part, other], axis=1)
        total = lax.dot_general(both, pair, dims, preferred_element_type=jnp.float32)
        if lines == ny:
            gram[ch, c] = total.reshape(ny, nz, rows, inputs)
        else:
            gram[ch, c, first] = total.reshape(nz, rows, inputs)

    def send_ends(at, ch, s, d):
        if d > 0:
            when(at == 0, lambda: z_copy(ch, s, d, 0).start())
        if d < nz - 1:
            when(at == nz - 1, lambda: z_copy(ch, s, d, 1).start())

    def issue(ch):
        known = isinstance(ch, int)
        if ny > 1 and (not known or ch < held):
            skip = [d for d in range(nz) if known and (ch, d) in wide]
            lines = [[d for d in far_first(nz, k) if d not in skip] for k in range(nz if static else 0)]
            for i in range(nz - len(skip)):
                y_copy(ch, pick(z, [line[i] for line in lines]) if static else i).start()
        for d in far_first(nz):
            if ny == 1 or (known and (ch, d) in wide):
                for s in range(ny):
                    send_ends(z, ch, s, d)

    def push(at):
        for ch, d in last_order(nz, at, range(held, chans)):
            y_copy(ch, d).start()

    def begin(ch):
        core_copy(ch).wait_recv()
        gram[ch, core] += from_core[ch]
        if isinstance(ch, int) or not wide:
            issue(ch)
        else:
            for k in range(2, chans - 1):
                pl.when(ch == k)(functools.partial(issue, k))

    def merge(at, ch, d):
        y_copy(ch, d).wait_recv()
        gram[ch, core, y, d] += from_y[ch, d]
        send_ends(at, ch, 0, d)

    def chain(at, ch, s, d, way):
        inside = at <= d if way == 0 else at >= d
        follows = at > 0 if way == 0 else at < nz - 1

        def act():
            z_copy(ch, s, d, way).wait_recv()
            into = block(ch, s, d)
            into[...] += from_z[unit(ch, s), d + 1 - way]
            when(at != d, lambda: z_copy(ch, s, d, way).start())

        if isinstance(at, int):
            when(inside and follows, act)
        else:
            when(jnp.logical_and(inside, follows), act)

    def cross(at, ch):
        y_copy(ch, at).start()

    def others(yy_range):
        return [(dz, yy, dc) for dz in range(nz) for yy in yy_range for dc in range(CORES) if dz or yy or dc]

    def place(at, dz, dy, dc):
        zz = (at + dz) % nz if isinstance(at, int) else lax.rem(at + dz, nz)
        return zz, (lax.rem(y + dy, ny) if ny > 1 else 0), lax.rem(core + dc, CORES)

    def flag_copy(at, hop):
        target = index_at(*place(at, *hop))
        return remote(packed, gathered.at[me], gs.at[0], gs.at[1], target)

    def flags_all():
        whole = gathered.at[pl.ds(0, count - 1)]
        return remote(whole, whole, gs.at[0], gs.at[1], partner)

    def blocks_of(shape):
        return mirrored.at[pl.ds(0, shape[0]), 0, pl.ds(0, shape[1])]

    def passes(at, ch):
        return ny > 1 and static and isinstance(ch, int) and ch < (late if 0 < at < nz - 1 else early)

    def wait_bytes(shape, send, recv):
        part = blocks_of(shape)
        return remote(part, part, send, recv, partner)

    near_hops = others((0,))
    far_hops = [(dz, 1, dc) for dz in range(nz) for dc in range(CORES)] if ny > 1 else []
    mine = z * CORES + core
    inner = pl.ds(CORES, column - 2 * CORES)

    def near_copy(at, ch, hop):
        zz, yy, cc = place(at, *hop)
        return remote(
            turned.at[ch, zz * CORES + cc], landed.at[ch, :, mine], fs.at[0], fr.at[ch], index_at(zz, yy, cc)
        )

    def near_wait(at, ch):
        count_in = column - 1 if ch < early else column - 2 * CORES - (0 < at < nz - 1)
        part = landed.at[ch, :, pl.ds(0, count_in)]
        return remote(part, part, fs.at[0], fr.at[ch], partner)

    def send_copy(at, ch, hop):
        zz, yy, cc = place(at, *hop)
        return remote(
            turned.at[ch, zz * CORES + cc, hop[1]], mirrored.at[ch, hop[1], mine], ds.at[ch - late], dr.at[ch - late],
            index_at(zz, yy, cc),
        )

    def bulk_copy(at, hop):
        zz, yy, cc = place(at, *hop)
        group = pl.ds(early, late - early)
        return remote(
            turned.at[group, zz * CORES + cc, hop[1]], mirrored.at[group, hop[1], mine], bs.at[hop[1]], br.at[hop[1]],
            index_at(zz, yy, cc),
        )

    def slots(ch):
        return pl.ds(0, column) if ch < early else inner

    def relay_copy(ch):
        part = slots(ch)
        return remote(
            landed.at[ch, 1, part], mirrored.at[ch, 1, part], xs.at[int(ch < early)], xr.at[int(ch < early)], opposite
        )

    def relay_all(group, part, slot):
        chunk = landed.at[group, 1, part]
        return remote(chunk, chunk, xs.at[slot], xr.at[slot], opposite)

    def near_out(ch):
        part = slots(ch)
        return pltpu.make_async_copy(landed.at[ch, 0, part], mirrored.at[ch, 0, part], ts.at[1 + 3 * int(ch < early)])

    def near_out_all(group, part, slot):
        return pltpu.make_async_copy(landed.at[group, 0, part], mirrored.at[group, 0, part], ts.at[1 + 3 * slot])

    def own_copy(ch):
        return pltpu.make_async_copy(turned.at[ch, mine, 0], mirrored.at[ch, 0, mine], ts.at[3])

    def keep_copy(ch):
        return pltpu.make_async_copy(gram.at[ch, core, y, z], kept.at[ch], ts.at[0])

    def scale_copy():
        return pltpu.make_async_copy(factor, scale, ts.at[2])

    def finish(at, ch):
        if isinstance(at, int) and (ch, at) in wide:
            y_copy(ch, at).wait_recv()
            gram[ch, core, y, at] += from_y[ch, at]
        keep_copy(ch).start()
        flipped = gram[ch, core, y, z].T
        each = rows // pack
        if each > 1:
            flipped = flipped.reshape(count, each, pack, rows)
            lane = lax.broadcasted_iota(jnp.int32, (count * pack, width), 1) // rows
            space = jnp.zeros((count * pack, width - rows), jnp.float32)
            total = None
            for a in range(each):
                piece = jnp.concatenate([flipped[:, a].reshape(count * pack, rows), space], axis=1)
                if a:
                    piece = pltpu.roll(piece, a * rows, 1)
                total = piece if total is None else jnp.where(lane == a, piece, total)
            flipped = total
        folded[...] = flipped.reshape(count, pack, width)
        for zz in range(nz):
            for cc in range(CORES):
                for dy in range(ny):
                    yy = lax.rem(y + dy, ny) if ny > 1 else 0
                    turned[ch, zz * CORES + cc, dy] = folded[owned[index_at(zz, yy, cc)]]
        if passes(at, ch):
            landed[ch, :, mine] = turned[ch, mine]
            for hop in near_hops:
                near_copy(at, ch, hop).start()
            return
        own_copy(ch).start()
        if not isinstance(ch, int) or ch >= late:
            hops = near_hops + far_hops
            if isinstance(at, int):
                hops.sort(key=lambda hop: (-abs((at + hop[0]) % nz - at), (at + hop[0]) % nz))
            for hop in hops:
                send_copy(at, ch, hop).start()

    def bulk(at):
        for hop in sorted(near_hops + far_hops, key=lambda hop: abs((at + hop[0]) % nz - at)):
            bulk_copy(at, hop).start()

    def relay(at):
        for ch in range(late):
            near_wait(at, ch).wait_recv()
            near_out(ch).start()
            relay_copy(ch).start()

    def send_flags(at):
        for hop in others(range(ny)):
            flag_copy(at, hop).start()

    def make_scale():
        flags_all().wait_recv()
        for index in range(count):
            value = jnp.where(me == index, packed[...], gathered[index])
            words_all[index * subs : (index + 1) * subs, :] = value[:subs, :words]
        every = words_all[...]
        slots = count * subs
        broad = max(span, 128)
        lane = lax.broadcasted_iota(jnp.int32, (slots, broad), 1)
        columns = []
        for word in range(0, words, broad // span):
            value = jnp.broadcast_to(every[:, word : word + 1], (slots, broad))
            for extra in range(1, broad // span):
                value = jnp.where(lane >= extra * span, every[:, word + extra : word + extra + 1], value)
            bits = jnp.right_shift(value, (lane % span) // 2)
            columns.append(jnp.bitwise_and(bits, 1).astype(jnp.float32))
        good = jnp.concatenate(columns, axis=1).astype(jnp.bfloat16)
        counts = lax.dot_general(good, good, (((0,), (0,)), ((), ())), preferred_element_type=jnp.float32)
        pairs[...] = counts.reshape(count, rows, inputs)
        factor[...] = 0.5 / jnp.maximum(length * pairs[owned[me]], 1.0)
        scale_copy().start()

    def wait_sent(ch, d, way):
        z_copy(ch, 0, d, way).wait_send()

    def finale(at):
        core_all().wait_send()
        for ch in range(chans):
            if ny > 1:
                y_all(ch, sum((ch, d) not in wide or d == at for d in range(nz))).wait_send()
            if static:
                for s in range(2 if ch in mixed else 1):
                    for way, line in ((0, range(at + 1, nz)), (1, range(at))):
                        blocks = sum(s == 0 or (ch, d) in wide for d in line)
                        if blocks:
                            z_all(way, unit(ch, s), blocks).wait_send()
            else:
                for d in range(nz):
                    when(at < d, functools.partial(wait_sent, ch, d, 0))
                    when(at > d, functools.partial(wait_sent, ch, d, 1))
        flags_all().wait_send()
        pltpu.make_async_copy(from_y.at[:, 0], kept, ts.at[0]).wait()
        scale_copy().wait()
        if late:
            ends = 2 * CORES
            inside = 0 < at < nz - 1
            groups = [(pl.ds(early, late - early), inner, 0), (pl.ds(0, early), pl.ds(0, column), 1)]
            for group in groups:
                if group[0].size:
                    near_out_all(*group).wait()
                    relay_all(*group).wait()
            passed = late if inside else early
            if passed:
                part = turned.at[pl.ds(0, passed), pl.ds(0, column - 1)]
                remote(part, part, fs.at[0], fr.at[0], partner).wait_send()
            if early < late:
                if not inside:
                    wait_bytes((late - early, column - 1), bs.at[0], br.at[0]).wait_send()
                    wait_bytes((late - early, column), bs.at[1], br.at[1]).wait_send()
                wait_bytes((late - early, ends - (not inside)), bs.at[0], br.at[0]).wait_recv()
                wait_bytes((late - early, ends), bs.at[1], br.at[1]).wait_recv()
            owned_blocks = chans - passed
        else:
            owned_blocks = chans
        pltpu.make_async_copy(turned.at[pl.ds(0, owned_blocks), 0, 0], mirrored.at[pl.ds(0, owned_blocks), 0, 0], ts.at[3]).wait()
        whole = pl.ds(0, count - 1)
        for ch in range(late, chans):
            remote(folded.at[whole], folded.at[whole], ds.at[ch - late], dr.at[ch - late], partner).wait()

    prepare(0)
    turns = [lax.rem(core + 1 + turn, CORES) for turn in range(CORES)]
    amount = 1 + (ny > 1) + (z > 0).astype(jnp.int32) + (z < nz - 1).astype(jnp.int32)
    if ny > 1:
        for slot, yy in ((0, 1 - y), (chans, y)):
            multiply(0, turns[0], yy, 1)
            if slot == 0:
                pl.semaphore_wait(barrier, amount)
            half_copy(0, yy, slot).start()
    else:
        multiply(0, turns[0], 0, ny)
        pl.semaphore_wait(barrier, amount)
        core_copy(0).start()
    prepare(1, 1)
    multiply(1, turns[0], 0, ny, 1)
    core_copy(1).start()
    multiply(0, turns[1], 0, ny)

    def compute(ch):
        prepare(ch)
        multiply(ch, turns[0], 0, ny)
        core_copy(ch).start()
        multiply(ch, turns[1], 0, ny)

    if ny > 1:
        for slot, yy in ((0, 1 - y), (chans, y)):
            half_copy(0, yy, slot).wait_recv()
            gram[0, core, yy] += from_core[0, yy]
            if slot == 0:
                issue(0)
    else:
        begin(0)
    multiply(1, turns[1], 0, ny, 1)
    begin(1)

    def body(ch, carry):
        compute(ch)
        pl.when(ch > 2)(lambda: begin(ch - 1))
        return carry

    lax.fori_loop(2, chans, body, 0)
    begin(chans - 1)

    if static:
        for at, events in enumerate(plan(nz, ny, chans, wide, held, early, late)):

            def play(at=at, events=events):
                acts = {"merge": merge, "chain": chain, "cross": cross, "finish": finish, "push": push, "relay": relay, "bulk": bulk}
                fresh = True
                for name, args in events:
                    acts[name](at, *args)
                    if name == "finish" and fresh:
                        fresh = False
                        send_flags(at)
                make_scale()
                finale(at)

            pl.when(z == at)(play)
    else:

        def line(ch, carry):
            for d in far_first(nz) if ny > 1 else ():
                merge(z, ch, d)
            for i in range(nz):
                for way, d in ((0, nz - 1 - i), (1, i)):
                    chain(z, ch, 0, d, way)
            finish(z, ch)
            return carry

        lax.fori_loop(0, chans, line, 0)
        send_flags(z)
        make_scale()
        finale(z)


def assemble(ny, step, owned_in, kept, mirrored, scale, out, owned, own, other, factors, result, holder, os, ms, rs, fs):
    chans, count, pack, width = mirrored.shape
    rows, inputs = scale.shape
    column = count // ny
    each = rows // pack
    y = lax.rem(lax.axis_index("tm") // CORES, ny)

    def fetch(part):
        group = pl.ds(part * step, step)
        return (
            pltpu.make_async_copy(mirrored.at[group], other.at[group], ms.at[part]),
            pltpu.make_async_copy(kept.at[group], own.at[group], os.at[part]),
        )

    scale_copy = pltpu.make_async_copy(scale, factors, fs.at[0])
    owned_copy = pltpu.make_async_copy(owned_in, owned, fs.at[1])
    owned_copy.start()
    scale_copy.start()
    for part in range(chans // step):
        for copy in fetch(part):
            copy.start()
    owned_copy.wait()
    for k in range(count):
        plane, rest = divmod(k, ny * CORES)
        yy, cc = divmod(rest, CORES)
        side = lax.rem(y + yy, ny) if ny > 1 else 0
        holder[owned[k]] = side * column + plane * CORES + cc
    per = 128 // rows
    lane = lax.broadcasted_iota(jnp.int32, (pack, 128), 1) // rows
    scale_copy.wait()
    factor = factors[...]
    for ch in range(chans):
        if ch % step == 0:
            for copy in fetch(ch // step):
                copy.wait()
        mirror = []
        for group in range(count // per):
            pieces = []
            for u in range(per):
                index = holder[group * per + u]
                pieces.append(other[ch, index])
            if each == 1:
                total = None
                for u, piece in enumerate(pieces):
                    piece = jnp.concatenate([piece, jnp.zeros((rows, 128 - rows), piece.dtype)], axis=1)
                    piece = pltpu.roll(piece, u * rows, 1) if u else piece
                    total = piece if total is None else jnp.where(lane == u, piece, total)
                mirror.append(total)
                continue
            turns = []
            for shift in range(per):
                total = pieces[shift]
                for v in range(1, per):
                    total = jnp.where(lane == v, pieces[(v + shift) % per], total)
                turns.append(pltpu.roll(total, shift * rows, 1) if shift else total)
            parts = []
            for a in range(each):
                total = turns[-a % per]
                for u in range(1, per):
                    total = jnp.where(lane == u, turns[(u - a) % per], total)
                parts.append(total)
            mirror.append(jnp.concatenate(parts, axis=0))
        left = own[ch]
        right = jnp.concatenate(mirror, axis=1)
        result[:, ch, 0, :] = (left + right) * factor
        result[:, ch, 1, :] = (left - right) * factor
        if ch % step == step - 1:
            group = pl.ds(ch + 1 - step, step)
            pltpu.make_async_copy(result.at[:, group], out.at[:, group], rs.at[0]).start()
    pltpu.make_async_copy(result, out, rs.at[0]).wait()


def shards(nz, ny, voltages, antenna_flags, owned_tile):
    count = nz * ny * CORES
    column = nz * CORES
    chans, _, inputs, samples = voltages.shape
    rows = inputs // count
    static = nz <= STATIC
    wide = frozenset((ch, d) for ch, d in WIDE(nz) if ch < chans) if ny > 1 and static else frozenset()
    held = chans - HELD if wide else chans
    late = chans - DIRECT if wide else 0
    early = min(EARLY, late)
    extra = len({ch for ch, _ in wide})
    held_type = jnp.bfloat16 if rows % 16 == 0 else jnp.float32
    each = max(1, 128 // rows)
    each = each if rows % (8 * each) == 0 else 1
    pack, width = rows // each, rows * each
    vmem = pl.BlockSpec(memory_space=pltpu.VMEM)
    smem = pl.BlockSpec(memory_space=pltpu.SMEM)
    hbm = pl.BlockSpec(memory_space=pltpu.HBM)
    dma = pltpu.SemaphoreType.DMA
    sizes = antenna_flags.shape
    kept, mirrored, scale = pl.pallas_call(
        functools.partial(kernel, nz, ny, wide, held, early, late),
        out_shape=(
            jax.ShapeDtypeStruct((chans, rows, inputs), jnp.float32),
            jax.ShapeDtypeStruct((chans, ny, column, pack, width), jnp.float32),
            jax.ShapeDtypeStruct((rows, inputs), jnp.float32),
        ),
        in_specs=[hbm, hbm, hbm],
        out_specs=(hbm, hbm, hbm),
        scratch_shapes=[
            pltpu.SMEM(owned_tile.shape, jnp.int32),
            pltpu.SMEM(sizes, jnp.int32),
            pltpu.VMEM(sizes, jnp.int32),
            pltpu.VMEM((chans, 2, count, rows, samples), voltages.dtype),
            pltpu.VMEM((count * sizes[0], sizes[1]), jnp.int32),
            pltpu.VMEM((count, rows, samples), held_type),
            pltpu.VMEM((2, count, rows, 2 * samples), held_type),
            pltpu.VMEM((count // CORES, rows, 2 * samples), held_type),
            pltpu.VMEM((chans, CORES, ny, nz, rows, inputs), jnp.float32),
            pltpu.VMEM((chans, ny, nz, rows, inputs), jnp.float32),
            pltpu.VMEM((chans, nz, rows, inputs), jnp.float32),
            pltpu.VMEM((chans + extra, nz + 1, rows, inputs), jnp.float32),
            pltpu.VMEM((chans, column, ny, pack, width), jnp.float32),
            pltpu.VMEM((count, pack, width), jnp.float32),
            pltpu.VMEM((max(late, 1), ny, column, pack, width), jnp.float32),
            pltpu.VMEM((rows, inputs), jnp.float32),
            pltpu.VMEM((count, rows, inputs), jnp.float32),
            pltpu.VMEM((count,) + sizes, jnp.int32),
            dma((chans,)), dma((1,)), dma((chans + 1,)), dma((chans,)), dma((chans, nz)),
            dma((2, chans + extra, 1 if static else nz)), dma((chans + extra, nz + 1)),
            dma((1,)), dma((max(late, 1),)), dma((chans - late,)), dma((chans - late,)), dma((2,)), dma((2,)), dma((2,)), dma((2,)), dma((2,)), dma((5,)), dma((3,)),
        ],
        compiler_params=pltpu.CompilerParams(
            collective_id=0, has_side_effects=True, vmem_limit_bytes=60 * 1024 * 1024
        ),
    )(owned_tile, antenna_flags, voltages.reshape(chans, 2, count, rows, samples))
    step = 2 if chans % 2 == 0 else 1
    return pl.pallas_call(
        functools.partial(assemble, ny, step),
        out_shape=jax.ShapeDtypeStruct((rows, chans, 2, inputs), jnp.float32),
        in_specs=[hbm, hbm, hbm, hbm],
        out_specs=hbm,
        scratch_shapes=[
            pltpu.SMEM((count,), jnp.int32),
            pltpu.VMEM((chans, rows, inputs), jnp.float32),
            pltpu.VMEM((chans, count, pack, width), jnp.float32),
            pltpu.VMEM((rows, inputs), jnp.float32),
            pltpu.VMEM((rows, chans, 2, inputs), jnp.float32),
            pltpu.SMEM((count,), jnp.int32),
            dma((chans // step,)), dma((chans // step,)), dma((1,)), dma((2,)),
        ],
    )(owned_tile, kept, mirrored.reshape(chans, count, pack, width), scale)


def solution(mesh):
    nz, ny = grid_of(mesh)
    return jax.shard_map(
        functools.partial(shards, nz, ny),
        mesh=mesh,
        in_specs=(P("band", None, None, "tm"), P("tm", "band"), P()),
        out_specs=P("tm", "band", None, None),
        check_vma=False,
    )
```

```python
import functools
import heapq

import jax
import jax.numpy as jnp
from jax import lax
from jax.experimental import pallas as pl
from jax.experimental.pallas import tpu as pltpu
from jax.sharding import PartitionSpec as P

MESH = pl.DeviceIdType.MESH
CORES = 2
BLOCK = 1.42
HOP = 2.0
FIRST = 4.0
START = 12.5
SLACK = 3.0
LATE = 7.0
STATIC = 4
HELD = 3
DIRECT = 3
EARLY = 3


def WIDE(nz):
    return {(1, d) for d in range(nz)}


def grid_of(mesh):
    count = mesh.shape["tm"]
    ny = 2 if mesh.shape["band"] < 4 and count % (4 * CORES) == 0 else 1
    return count // (ny * CORES), ny


def far_first(nz, z=None):
    middle = (nz - 1) / 2 if z is None else z
    return sorted(range(nz), key=lambda d: (-abs(d - middle), d))


def last_order(nz, z, channels):
    ranks = list(enumerate(far_first(nz, z)))
    return [(ch, d) for _, _, ch, d in sorted((i + ch, -ch, ch, d) for ch in channels for i, d in ranks)]


def pick(z, values):
    if isinstance(z, int):
        return values[z]
    return sum(jnp.where(z == k, value, 0) for k, value in enumerate(values))


def when(condition, act):
    if isinstance(condition, bool):
        if condition:
            act()
    else:
        pl.when(condition)(act)


def plan(nz, ny, chans, wide, held, early, late):
    order = far_first(nz)
    mixed = sorted({ch for ch, _ in wide})
    events = [[] for _ in range(nz)]
    free = [[0.0, 0.0] for _ in range(nz)]
    queue, merged, landed, ended = [], set(), set(), {}
    sent = {}
    serial = iter(range(1 << 30))

    def add(time, *what):
        heapq.heappush(queue, (time if what[0] == "own" else max(time, START), next(serial), what))

    def note(z, time, name, *args):
        events[z].append((time, next(serial), name, args))

    def slack(ch):
        return SLACK if ch < chans - 2 else 0.0

    def forward(now, z, ch, s, d, way):
        free[z][way] = max(free[z][way], now) + BLOCK
        add(free[z][way] + HOP, "land", z + 1 - 2 * way, ch, s, d, way)

    def own(now, z, ch, s, d):
        merged.add((z, ch, s, d))
        if z == 0 and d > 0:
            forward(now, z, ch, s, d, 0)
        if z == nz - 1 and d < nz - 1:
            forward(now, z, ch, s, d, 1)
        for way in range(2):
            if (z, ch, s, d, way) in landed:
                join(now, z, ch, s, d, way)

    def join(now, z, ch, s, d, way):
        if z != d:
            note(z, now, "chain", ch, s, d, way)
            forward(now, z, ch, s, d, way)
            return
        note(z, now + slack(ch), "chain", ch, s, d, way)
        ended[z, ch, s] = ended.get((z, ch, s), 0) + 1
        if ended[z, ch, s] < (2 if 0 < z < nz - 1 else 1):
            return
        if s == 1:
            note(z, now + slack(ch), "cross", ch)
            pushes[z] = max(pushes[z], now + slack(ch))
            add(max(now, crossing) + BLOCK * len(mixed) + HOP, "whole", z, ch)
        else:
            add(now, "whole", z, ch)

    clock = FIRST
    crossing = 0.0
    pushes = [0.0] * nz
    for ch in range(chans):
        if ch == held:
            crossing = clock
            clock += BLOCK * len(mixed)
            for z in range(nz):
                for i, (each, d) in enumerate(last_order(nz, z, range(held, chans))):
                    add(clock + BLOCK * (i + 1) + HOP, "merge", z, each, d)
            clock += BLOCK * nz * (chans - held)
            break
        steps = 0
        for z in range(nz):
            line = [d for d in far_first(nz, z) if (ch, d) not in wide and ny > 1]
            steps = len(line)
            for i, d in enumerate(line):
                add(clock + BLOCK * (i + 1) + HOP, "merge", z, ch, d)
            for d in order:
                if d not in line:
                    for s in range(ny):
                        add(FIRST + 1.5 * ch, "own", z, ch, s, d)
        clock += BLOCK * steps
    parts = {}
    while queue:
        now, _, (name, z, ch, *rest) = heapq.heappop(queue)
        if name == "merge":
            note(z, now, "merge", ch, *rest)
            own(now, z, ch, 0, *rest)
        elif name == "own":
            own(now, z, ch, *rest)
        elif name == "land":
            landed.add((z, ch, *rest))
            if (z, ch, *rest[:2]) in merged:
                join(now, z, ch, *rest)
        else:
            parts[z, ch] = parts.get((z, ch), 0) + 1
            if parts[z, ch] == (2 if (ch, z) in wide else 1):
                note(z, now + slack(ch), "finish", ch)
                last = now + slack(ch)
                if ch < late:
                    sent[z] = max(sent.get(z, 0.0), last)
                if 0 < z < nz - 1 or not early <= ch < late:
                    for way, planes in ((0, nz - 1 - z), (1, z)):
                        free[z][way] = max(free[z][way], now) + BLOCK * planes / nz
    for z in range(nz):
        if late:
            note(z, max(max(sent.values()), clock) + HOP + 0.05, "relay")
            if z in (0, nz - 1) and early < late:
                note(z, max(sent[z], clock - 1.0), "bulk")
        if ny > 1 and held < chans:
            note(z, pushes[z], "push")
        events[z].sort()
    return [[(name, args) for _, _, name, args in line] for line in events]


def kernel(nz, ny, wide, held, early, late, owned_in, flags_in, volts, kept, mirrored, scale, owned, flags, packed, loaded, words_all, mask, natural, left,
           gram, from_core, from_y, from_z, turned, folded, landed, factor, pairs, gathered,
           ls, cs, cr, ys, yr, zs, zr, fs, fr, ds, dr, bs, br, xs, xr, gs, ts, hs):
    count = nz * ny * CORES
    column = nz * CORES
    chans, _, tiles, rows, samples = volts.shape
    inputs = tiles * rows
    pack, width = folded.shape[1:]
    static = nz <= STATIC
    mixed = sorted({ch for ch, _ in wide})
    me = lax.axis_index("tm")
    core = lax.rem(me, CORES)
    y = lax.rem(me // CORES, ny)
    z = me // (CORES * ny)

    def index_at(zz, yy, cc):
        return (zz * ny + yy) * CORES + cc

    partner = index_at(z, y, 1 - core)
    opposite = index_at(z, 1 - y if ny > 1 else 0, core)
    barrier = pltpu.get_barrier_semaphore()

    def greet(target):
        pl.semaphore_signal(barrier, inc=1, device_id={"tm": target}, device_id_type=MESH)

    greet(partner)
    if ny > 1:
        greet(opposite)
    pl.when(z > 0)(lambda: greet(index_at(z - 1, y, core)))
    pl.when(z < nz - 1)(lambda: greet(index_at(z + 1, y, core)))

    def load(ch):
        return pltpu.make_async_copy(volts.at[ch], loaded.at[ch], ls.at[ch])

    small = [
        pltpu.make_async_copy(flags_in, flags, hs.at[0]),
        pltpu.make_async_copy(owned_in, owned, hs.at[1]),
        pltpu.make_async_copy(flags_in, packed, hs.at[2]),
    ]
    for copy in small:
        copy.start()
    load(0).start()
    for copy in small:
        copy.wait()
    for ch in range(1, chans):
        load(ch).start()

    subs, words = flags.shape
    length = samples // subs
    span = inputs // words
    shift = lax.broadcasted_iota(jnp.int32, (span, length), 0) // 2
    for word in range(words):
        for sub in range(subs):
            bits = jnp.right_shift(jnp.full((span, length), flags[sub, word], jnp.int32), shift)
            good = jnp.bitwise_and(bits, 1).astype(jnp.float32).astype(mask.dtype)
            good = good.reshape(span // rows, rows, length)
            mask[word * (span // rows) : (word + 1) * (span // rows), :, sub * length : (sub + 1) * length] = good

    def remote(src, dst, send, recv, target):
        return pltpu.make_async_remote_copy(
            src_ref=src, dst_ref=dst, send_sem=send, recv_sem=recv,
            device_id={"tm": target}, device_id_type=MESH,
        )

    def core_copy(ch):
        return remote(gram.at[ch, 1 - core], from_core.at[ch], cs.at[0], cr.at[ch], partner)

    def half_copy(ch, yy, slot):
        return remote(gram.at[ch, 1 - core, yy], from_core.at[ch, yy], cs.at[0], cr.at[slot], partner)

    def core_all():
        return remote(from_core, from_core, cs.at[0], cr.at[0], partner)

    def y_copy(ch, d):
        return remote(gram.at[ch, core, 1 - y, d], from_y.at[ch, d], ys.at[ch], yr.at[ch, d], opposite)

    def y_all(ch, blocks):
        part = from_y.at[ch, pl.ds(0, blocks)]
        return remote(part, part, ys.at[ch], yr.at[ch, 0], opposite)

    def block(ch, s, d):
        return gram.at[ch, core, lax.rem(y + s, ny) if ny > 1 else 0, d]

    def unit(ch, s):
        return chans + mixed.index(ch) if s else ch

    def sent_slot(ch, s):
        return (1 + mixed.index(ch) if s else 0) if static else ch

    def z_copy(ch, s, d, way):
        u, slot = unit(ch, s), d + 1 - way
        return remote(
            block(ch, s, d), from_z.at[u, slot], zs.at[way, sent_slot(ch, s), 0 if static else d], zr.at[u, slot],
            index_at(z + 1 - 2 * way, y, core),
        )

    def z_all(way, slot, units, blocks):
        part = from_z.at[pl.ds(0, units), pl.ds(0, blocks)]
        return remote(part, part, zs.at[way, slot, 0], zr.at[0, 0], partner)

    def prepare(ch, slot=0):
        load(ch).wait()
        for part in range(2):
            value = loaded[ch, part].astype(mask.dtype) * mask[...]
            natural[slot, :, :, part * samples : (part + 1) * samples] = value

    def multiply(ch, c, first, lines, slot=0):
        pair = natural[slot].reshape(inputs, 2 * samples).astype(jnp.bfloat16)
        pair = jnp.concatenate([pair, pair], axis=1)
        for yy in range(lines):
            for zz in range(nz):
                left[yy * nz + zz] = natural[slot, owned[index_at(zz, first + yy, c)]]
        part = left[0 : lines * nz].reshape(lines * nz * rows, 2 * samples).astype(jnp.bfloat16)
        other = jnp.concatenate([part[:, samples:], -part[:, :samples]], axis=1)
        dims = (((1,), (1,)), ((), ()))
        both = jnp.concatenate([part, other], axis=1)
        total = lax.dot_general(both, pair, dims, preferred_element_type=jnp.float32)
        if lines == ny:
            gram[ch, c] = total.reshape(ny, nz, rows, inputs)
        else:
            gram[ch, c, first] = total.reshape(nz, rows, inputs)

    def send_ends(at, ch, s, d):
        if d > 0:
            when(at == 0, lambda: z_copy(ch, s, d, 0).start())
        if d < nz - 1:
            when(at == nz - 1, lambda: z_copy(ch, s, d, 1).start())

    def issue(ch):
        known = isinstance(ch, int)
        if ny > 1 and (not known or ch < held):
            skip = [d for d in range(nz) if known and (ch, d) in wide]
            lines = [[d for d in far_first(nz, k) if d not in skip] for k in range(nz if static else 0)]
            for i in range(nz - len(skip)):
                y_copy(ch, pick(z, [line[i] for line in lines]) if static else i).start()
        for d in far_first(nz):
            if ny == 1 or (known and (ch, d) in wide):
                for s in range(ny):
                    send_ends(z, ch, s, d)

    def push(at):
        for ch, d in last_order(nz, at, range(held, chans)):
            y_copy(ch, d).start()

    def begin(ch):
        core_copy(ch).wait_recv()
        gram[ch, core] += from_core[ch]
        if isinstance(ch, int) or not wide:
            issue(ch)
        else:
            for k in range(2, chans - 1):
                pl.when(ch == k)(functools.partial(issue, k))

    def merge(at, ch, d):
        y_copy(ch, d).wait_recv()
        gram[ch, core, y, d] += from_y[ch, d]
        send_ends(at, ch, 0, d)

    def chain(at, ch, s, d, way):
        inside = at <= d if way == 0 else at >= d
        follows = at > 0 if way == 0 else at < nz - 1

        def act():
            z_copy(ch, s, d, way).wait_recv()
            into = block(ch, s, d)
            into[...] += from_z[unit(ch, s), d + 1 - way]
            when(at != d, lambda: z_copy(ch, s, d, way).start())

        if isinstance(at, int):
            when(inside and follows, act)
        else:
            when(jnp.logical_and(inside, follows), act)

    def cross(at, ch):
        y_copy(ch, at).start()

    def others(yy_range):
        return [(dz, yy, dc) for dz in range(nz) for yy in yy_range for dc in range(CORES) if dz or yy or dc]

    def place(at, dz, dy, dc):
        zz = (at + dz) % nz if isinstance(at, int) else lax.rem(at + dz, nz)
        return zz, (lax.rem(y + dy, ny) if ny > 1 else 0), lax.rem(core + dc, CORES)

    def flag_copy(at, hop):
        target = index_at(*place(at, *hop))
        return remote(packed, gathered.at[me], gs.at[0], gs.at[1], target)

    def flags_all():
        whole = gathered.at[pl.ds(0, count - 1)]
        return remote(whole, whole, gs.at[0], gs.at[1], partner)

    def blocks_of(shape):
        return mirrored.at[pl.ds(0, shape[0]), 0, pl.ds(0, shape[1])]

    def passes(at, ch):
        return ny > 1 and static and isinstance(ch, int) and ch < (late if 0 < at < nz - 1 else early)

    def wait_bytes(shape, send, recv):
        part = blocks_of(shape)
        return remote(part, part, send, recv, partner)

    near_hops = others((0,))
    far_hops = [(dz, 1, dc) for dz in range(nz) for dc in range(CORES)] if ny > 1 else []
    mine = z * CORES + core
    inner = pl.ds(CORES, column - 2 * CORES)

    def near_copy(at, ch, hop):
        zz, yy, cc = place(at, *hop)
        return remote(
            turned.at[ch, zz * CORES + cc], landed.at[ch, :, mine], fs.at[0], fr.at[ch], index_at(zz, yy, cc)
        )

    def near_wait(at, ch):
        count_in = column - 1 if ch < early else column - 2 * CORES - (0 < at < nz - 1)
        part = landed.at[ch, :, pl.ds(0, count_in)]
        return remote(part, part, fs.at[0], fr.at[ch], partner)

    def send_copy(at, ch, hop):
        zz, yy, cc = place(at, *hop)
        return remote(
            turned.at[ch, zz * CORES + cc, hop[1]], mirrored.at[ch, hop[1], mine], ds.at[ch - late], dr.at[ch - late],
            index_at(zz, yy, cc),
        )

    def bulk_copy(at, hop):
        zz, yy, cc = place(at, *hop)
        group = pl.ds(early, late - early)
        return remote(
            turned.at[group, zz * CORES + cc, hop[1]], mirrored.at[group, hop[1], mine], bs.at[hop[1]], br.at[hop[1]],
            index_at(zz, yy, cc),
        )

    def slots(ch):
        return pl.ds(0, column) if ch < early else inner

    def relay_copy(ch):
        part = slots(ch)
        return remote(
            landed.at[ch, 1, part], mirrored.at[ch, 1, part], xs.at[int(ch < early)], xr.at[int(ch < early)], opposite
        )

    def relay_all(group, part, slot):
        chunk = landed.at[group, 1, part]
        return remote(chunk, chunk, xs.at[slot], xr.at[slot], opposite)

    def near_out(ch):
        part = slots(ch)
        return pltpu.make_async_copy(landed.at[ch, 0, part], mirrored.at[ch, 0, part], ts.at[1 + 3 * int(ch < early)])

    def near_out_all(group, part, slot):
        return pltpu.make_async_copy(landed.at[group, 0, part], mirrored.at[group, 0, part], ts.at[1 + 3 * slot])

    def own_copy(ch):
        return pltpu.make_async_copy(turned.at[ch, mine, 0], mirrored.at[ch, 0, mine], ts.at[3])

    def keep_copy(ch):
        return pltpu.make_async_copy(gram.at[ch, core, y, z], kept.at[ch], ts.at[0])

    def scale_copy():
        return pltpu.make_async_copy(factor, scale, ts.at[2])

    def finish(at, ch):
        if isinstance(at, int) and (ch, at) in wide:
            y_copy(ch, at).wait_recv()
            gram[ch, core, y, at] += from_y[ch, at]
        keep_copy(ch).start()
        flipped = gram[ch, core, y, z].T
        each = rows // pack
        if each > 1:
            flipped = flipped.reshape(count, each, pack, rows)
            lane = lax.broadcasted_iota(jnp.int32, (count * pack, width), 1) // rows
            space = jnp.zeros((count * pack, width - rows), jnp.float32)
            total = None
            for a in range(each):
                piece = jnp.concatenate([flipped[:, a].reshape(count * pack, rows), space], axis=1)
                if a:
                    piece = pltpu.roll(piece, a * rows, 1)
                total = piece if total is None else jnp.where(lane == a, piece, total)
            flipped = total
        folded[...] = flipped.reshape(count, pack, width)
        for zz in range(nz):
            for cc in range(CORES):
                for dy in range(ny):
                    yy = lax.rem(y + dy, ny) if ny > 1 else 0
                    turned[ch, zz * CORES + cc, dy] = folded[owned[index_at(zz, yy, cc)]]
        if passes(at, ch):
            landed[ch, :, mine] = turned[ch, mine]
            for hop in near_hops:
                near_copy(at, ch, hop).start()
            return
        own_copy(ch).start()
        if not isinstance(ch, int) or ch >= late:
            hops = near_hops + far_hops
            if isinstance(at, int):
                hops.sort(key=lambda hop: (-abs((at + hop[0]) % nz - at), (at + hop[0]) % nz))
            for hop in hops:
                send_copy(at, ch, hop).start()

    def bulk(at):
        for hop in sorted(near_hops + far_hops, key=lambda hop: abs((at + hop[0]) % nz - at)):
            bulk_copy(at, hop).start()

    def relay(at):
        for ch in range(late):
            near_wait(at, ch).wait_recv()
            near_out(ch).start()
            relay_copy(ch).start()

    def send_flags(at):
        for hop in others(range(ny)):
            flag_copy(at, hop).start()

    def make_scale():
        flags_all().wait_recv()
        for index in range(count):
            value = jnp.where(me == index, packed[...], gathered[index])
            words_all[index * subs : (index + 1) * subs, :] = value[:subs, :words]
        every = words_all[...]
        slots = count * subs
        broad = max(span, 128)
        lane = lax.broadcasted_iota(jnp.int32, (slots, broad), 1)
        columns = []
        for word in range(0, words, broad // span):
            value = jnp.broadcast_to(every[:, word : word + 1], (slots, broad))
            for extra in range(1, broad // span):
                value = jnp.where(lane >= extra * span, every[:, word + extra : word + extra + 1], value)
            bits = jnp.right_shift(value, (lane % span) // 2)
            columns.append(jnp.bitwise_and(bits, 1).astype(jnp.float32))
        good = jnp.concatenate(columns, axis=1).astype(jnp.bfloat16)
        counts = lax.dot_general(good, good, (((0,), (0,)), ((), ())), preferred_element_type=jnp.float32)
        pairs[...] = counts.reshape(count, rows, inputs)
        factor[...] = 0.5 / jnp.maximum(length * pairs[owned[me]], 1.0)
        scale_copy().start()

    def wait_sent(ch, d, way):
        z_copy(ch, 0, d, way).wait_send()

    def finale(at):
        core_all().wait_send()
        for ch in range(chans):
            if ny > 1:
                y_all(ch, sum((ch, d) not in wide or d == at for d in range(nz))).wait_send()
            if static:
                for way, line in ((0, range(at + 1, nz)), (1, range(at))):
                    if ch == 0 and line:
                        z_all(way, 0, chans, len(line)).wait_send()
                    blocks = sum((ch, d) in wide for d in line)
                    if blocks:
                        z_all(way, sent_slot(ch, 1), 1, blocks).wait_send()
            else:
                for d in range(nz):
                    when(at < d, functools.partial(wait_sent, ch, d, 0))
                    when(at > d, functools.partial(wait_sent, ch, d, 1))
        flags_all().wait_send()
        pltpu.make_async_copy(from_y.at[:, 0], kept, ts.at[0]).wait()
        scale_copy().wait()
        if late:
            ends = 2 * CORES
            inside = 0 < at < nz - 1
            groups = [(pl.ds(early, late - early), inner, 0), (pl.ds(0, early), pl.ds(0, column), 1)]
            for group in groups:
                if group[0].size:
                    near_out_all(*group).wait()
                    relay_all(*group).wait()
            passed = late if inside else early
            if passed:
                part = turned.at[pl.ds(0, passed), pl.ds(0, column - 1)]
                remote(part, part, fs.at[0], fr.at[0], partner).wait_send()
            if early < late:
                if not inside:
                    wait_bytes((late - early, column - 1), bs.at[0], br.at[0]).wait_send()
                    wait_bytes((late - early, column), bs.at[1], br.at[1]).wait_send()
                wait_bytes((late - early, ends - (not inside)), bs.at[0], br.at[0]).wait_recv()
                wait_bytes((late - early, ends), bs.at[1], br.at[1]).wait_recv()
            owned_blocks = chans - passed
        else:
            owned_blocks = chans
        pltpu.make_async_copy(turned.at[pl.ds(0, owned_blocks), 0, 0], mirrored.at[pl.ds(0, owned_blocks), 0, 0], ts.at[3]).wait()
        whole = pl.ds(0, count - 1)
        for ch in range(late, chans):
            remote(folded.at[whole], folded.at[whole], ds.at[ch - late], dr.at[ch - late], partner).wait()

    prepare(0)
    turns = [lax.rem(core + 1 + turn, CORES) for turn in range(CORES)]
    amount = 1 + (ny > 1) + (z > 0).astype(jnp.int32) + (z < nz - 1).astype(jnp.int32)
    if ny > 1:
        for slot, yy in ((0, 1 - y), (chans, y)):
            multiply(0, turns[0], yy, 1)
            if slot == 0:
                pl.semaphore_wait(barrier, amount)
            half_copy(0, yy, slot).start()
    else:
        multiply(0, turns[0], 0, ny)
        pl.semaphore_wait(barrier, amount)
        core_copy(0).start()
    prepare(1, 1)
    multiply(1, turns[0], 0, ny, 1)
    core_copy(1).start()
    multiply(0, turns[1], 0, ny)

    def compute(ch):
        prepare(ch)
        multiply(ch, turns[0], 0, ny)
        core_copy(ch).start()
        multiply(ch, turns[1], 0, ny)

    if ny > 1:
        for slot, yy in ((0, 1 - y), (chans, y)):
            half_copy(0, yy, slot).wait_recv()
            gram[0, core, yy] += from_core[0, yy]
            if slot == 0:
                issue(0)
    else:
        begin(0)
    multiply(1, turns[1], 0, ny, 1)
    begin(1)

    def body(ch, carry):
        compute(ch)
        pl.when(ch > 2)(lambda: begin(ch - 1))
        return carry

    lax.fori_loop(2, chans, body, 0)
    begin(chans - 1)

    if static:
        for at, events in enumerate(plan(nz, ny, chans, wide, held, early, late)):

            def play(at=at, events=events):
                acts = {"merge": merge, "chain": chain, "cross": cross, "finish": finish, "push": push, "relay": relay, "bulk": bulk}
                fresh = True
                for name, args in events:
                    acts[name](at, *args)
                    if name == "finish" and fresh:
                        fresh = False
                        send_flags(at)
                make_scale()
                finale(at)

            pl.when(z == at)(play)
    else:

        def line(ch, carry):
            for d in far_first(nz) if ny > 1 else ():
                merge(z, ch, d)
            for i in range(nz):
                for way, d in ((0, nz - 1 - i), (1, i)):
                    chain(z, ch, 0, d, way)
            finish(z, ch)
            return carry

        lax.fori_loop(0, chans, line, 0)
        send_flags(z)
        make_scale()
        finale(z)


def assemble(ny, step, owned_in, kept, mirrored, scale, out, owned, own, other, factors, result, holder, os, ms, rs, fs):
    chans, count, pack, width = mirrored.shape
    rows, inputs = scale.shape
    column = count // ny
    each = rows // pack
    y = lax.rem(lax.axis_index("tm") // CORES, ny)

    def fetch(part):
        group = pl.ds(part * step, step)
        return (
            pltpu.make_async_copy(mirrored.at[group], other.at[group], ms.at[part]),
            pltpu.make_async_copy(kept.at[group], own.at[group], os.at[part]),
        )

    scale_copy = pltpu.make_async_copy(scale, factors, fs.at[0])
    owned_copy = pltpu.make_async_copy(owned_in, owned, fs.at[1])
    owned_copy.start()
    scale_copy.start()
    for part in range(chans // step):
        for copy in fetch(part):
            copy.start()
    owned_copy.wait()
    for k in range(count):
        plane, rest = divmod(k, ny * CORES)
        yy, cc = divmod(rest, CORES)
        side = lax.rem(y + yy, ny) if ny > 1 else 0
        holder[owned[k]] = side * column + plane * CORES + cc
    per = 128 // rows
    lane = lax.broadcasted_iota(jnp.int32, (pack, 128), 1) // rows
    scale_copy.wait()
    factor = factors[...]
    for ch in range(chans):
        if ch % step == 0:
            for copy in fetch(ch // step):
                copy.wait()
        mirror = []
        for group in range(count // per):
            pieces = []
            for u in range(per):
                index = holder[group * per + u]
                pieces.append(other[ch, index])
            if each == 1:
                total = None
                for u, piece in enumerate(pieces):
                    piece = jnp.concatenate([piece, jnp.zeros((rows, 128 - rows), piece.dtype)], axis=1)
                    piece = pltpu.roll(piece, u * rows, 1) if u else piece
                    total = piece if total is None else jnp.where(lane == u, piece, total)
                mirror.append(total)
                continue
            turns = []
            for shift in range(per):
                total = pieces[shift]
                for v in range(1, per):
                    total = jnp.where(lane == v, pieces[(v + shift) % per], total)
                turns.append(pltpu.roll(total, shift * rows, 1) if shift else total)
            parts = []
            for a in range(each):
                total = turns[-a % per]
                for u in range(1, per):
                    total = jnp.where(lane == u, turns[(u - a) % per], total)
                parts.append(total)
            mirror.append(jnp.concatenate(parts, axis=0))
        left = own[ch]
        right = jnp.concatenate(mirror, axis=1)
        result[:, ch, 0, :] = (left + right) * factor
        result[:, ch, 1, :] = (left - right) * factor
        if ch % step == step - 1:
            group = pl.ds(ch + 1 - step, step)
            pltpu.make_async_copy(result.at[:, group], out.at[:, group], rs.at[0]).start()
    pltpu.make_async_copy(result, out, rs.at[0]).wait()


def shards(nz, ny, voltages, antenna_flags, owned_tile):
    count = nz * ny * CORES
    column = nz * CORES
    chans, _, inputs, samples = voltages.shape
    rows = inputs // count
    static = nz <= STATIC
    wide = frozenset((ch, d) for ch, d in WIDE(nz) if ch < chans) if ny > 1 and static else frozenset()
    held = chans - HELD if wide else chans
    late = chans - DIRECT if wide else 0
    early = min(EARLY, late)
    extra = len({ch for ch, _ in wide})
    held_type = jnp.bfloat16 if rows % 16 == 0 else jnp.float32
    each = max(1, 128 // rows)
    each = each if rows % (8 * each) == 0 else 1
    pack, width = rows // each, rows * each
    vmem = pl.BlockSpec(memory_space=pltpu.VMEM)
    smem = pl.BlockSpec(memory_space=pltpu.SMEM)
    hbm = pl.BlockSpec(memory_space=pltpu.HBM)
    dma = pltpu.SemaphoreType.DMA
    sizes = antenna_flags.shape
    kept, mirrored, scale = pl.pallas_call(
        functools.partial(kernel, nz, ny, wide, held, early, late),
        out_shape=(
            jax.ShapeDtypeStruct((chans, rows, inputs), jnp.float32),
            jax.ShapeDtypeStruct((chans, ny, column, pack, width), jnp.float32),
            jax.ShapeDtypeStruct((rows, inputs), jnp.float32),
        ),
        in_specs=[hbm, hbm, hbm],
        out_specs=(hbm, hbm, hbm),
        scratch_shapes=[
            pltpu.SMEM(owned_tile.shape, jnp.int32),
            pltpu.SMEM(sizes, jnp.int32),
            pltpu.VMEM(sizes, jnp.int32),
            pltpu.VMEM((chans, 2, count, rows, samples), voltages.dtype),
            pltpu.VMEM((count * sizes[0], sizes[1]), jnp.int32),
            pltpu.VMEM((count, rows, samples), held_type),
            pltpu.VMEM((2, count, rows, 2 * samples), held_type),
            pltpu.VMEM((count // CORES, rows, 2 * samples), held_type),
            pltpu.VMEM((chans, CORES, ny, nz, rows, inputs), jnp.float32),
            pltpu.VMEM((chans, ny, nz, rows, inputs), jnp.float32),
            pltpu.VMEM((chans, nz, rows, inputs), jnp.float32),
            pltpu.VMEM((chans + extra, nz + 1, rows, inputs), jnp.float32),
            pltpu.VMEM((chans, column, ny, pack, width), jnp.float32),
            pltpu.VMEM((count, pack, width), jnp.float32),
            pltpu.VMEM((max(late, 1), ny, column, pack, width), jnp.float32),
            pltpu.VMEM((rows, inputs), jnp.float32),
            pltpu.VMEM((count, rows, inputs), jnp.float32),
            pltpu.VMEM((count,) + sizes, jnp.int32),
            dma((chans,)), dma((1,)), dma((chans + 1,)), dma((chans,)), dma((chans, nz)),
            dma((2, 1 + extra if static else chans, 1 if static else nz)), dma((chans + extra, nz + 1)),
            dma((1,)), dma((max(late, 1),)), dma((chans - late,)), dma((chans - late,)), dma((2,)), dma((2,)), dma((2,)), dma((2,)), dma((2,)), dma((5,)), dma((3,)),
        ],
        compiler_params=pltpu.CompilerParams(
            collective_id=0, has_side_effects=True, vmem_limit_bytes=60 * 1024 * 1024
        ),
    )(owned_tile, antenna_flags, voltages.reshape(chans, 2, count, rows, samples))
    step = 2 if chans % 2 == 0 else 1
    return pl.pallas_call(
        functools.partial(assemble, ny, step),
        out_shape=jax.ShapeDtypeStruct((rows, chans, 2, inputs), jnp.float32),
        in_specs=[hbm, hbm, hbm, hbm],
        out_specs=hbm,
        scratch_shapes=[
            pltpu.SMEM((count,), jnp.int32),
            pltpu.VMEM((chans, rows, inputs), jnp.float32),
            pltpu.VMEM((chans, count, pack, width), jnp.float32),
            pltpu.VMEM((rows, inputs), jnp.float32),
            pltpu.VMEM((rows, chans, 2, inputs), jnp.float32),
            pltpu.SMEM((count,), jnp.int32),
            dma((chans // step,)), dma((chans // step,)), dma((1,)), dma((2,)),
        ],
    )(owned_tile, kept, mirrored.reshape(chans, count, pack, width), scale)


def solution(mesh):
    nz, ny = grid_of(mesh)
    return jax.shard_map(
        functools.partial(shards, nz, ny),
        mesh=mesh,
        in_specs=(P("band", None, None, "tm"), P("tm", "band"), P()),
        out_specs=P("tm", "band", None, None),
        check_vma=False,
    )
```
